128 devices in a mesh: gx: 4 (over y), gy: 8 (over z_hi, x), gz: 4 (over z_lo, core).
Axes of the slice: x: 4, y: 4, z: 4 (z_hi: 2, z_lo: 2; z = z_hi * 2 + z_lo), core: 2. Of those that a mesh axis runs over, the one named last changes fastest.
Arguments:
- noisy_image: float32 [32, 256, 512], P('gz', 'gy', 'gx'), may hold values from -6 to 6
- fidelity: float32 [32, 256, 512], P('gz', 'gy', 'gx'), may hold values from 0.5 to 8
- primal_u: float32 [32, 256, 512], P('gz', 'gy', 'gx'), may hold values from -6 to 6
- primal_v: float32 [3, 32, 256, 512], P(None, 'gz', 'gy', 'gx'), may hold values from -2 to 2
- dual_p: float32 [3, 32, 256, 512], P(None, 'gz', 'gy', 'gx'), may hold values from -2.5 to 2.5
- dual_q: float32 [6, 32, 256, 512], P(None, 'gz', 'gy', 'gx'), may hold values from -2.5 to 2.5
Outputs:
- denoised: float32 [32, 256, 512], P('gz', 'gy', 'gx')
- vector_field: float32 [3, 32, 256, 512], P(None, 'gz', 'gy', 'gx')
- grad_dual: float32 [3, 32, 256, 512], P(None, 'gz', 'gy', 'gx')
- sym_dual: float32 [6, 32, 256, 512], P(None, 'gz', 'gy', 'gx')
The draws below stay inside these ranges and needn't reach their ends.
All inputs are finite; a program needn't handle non-finite values.
Results may differ from the reference program's by a relative error of at most 0.0001.
Values sent between devices are 32-bit elements; how exact they have to be, the bound alone decides.
A program may use at most 64 MiB of HBM per device.

```python
import math
import jax
import jax.numpy as jnp
from jax import lax

ITERS = 3
NX = 512
NY = 256
NZ = 32


def shard_levels(stream_key, shape, split, smallest, largest):
    def one(dim, shards_of):
        draws = jax.random.uniform(jax.random.fold_in(jax.random.fold_in(stream_key, 6), dim), (shards_of,), jnp.float32, smallest / len(split), largest / len(split))
        return jnp.repeat(jnp.exp(draws), shape[dim] // shards_of).reshape((-1,) + (1,) * (len(shape) - dim - 1))

    loudness = one(*split[0])
    for cut in split[1:]:
        loudness = loudness * one(*cut)
    return loudness


def bell_draw(own_key, shape, spread, limit, shards=(), kind=jnp.bfloat16):
    drawn = jax.random.normal(own_key, shape, jnp.float32) * spread
    if len(shards) > 0:
        drawn = shard_levels(own_key, shape, shards, -0.22, 0.18) * drawn
    return jnp.clip(drawn, min=-limit, max=limit).astype(kind)


def setup_inputs(seed: int = 0) -> dict:
    streams_of = jax.random.split(jax.random.key(seed), 7)
    noisy_image = bell_draw(streams_of[0], (NZ, NY, NX), 1.0, 6.0, ((0, 4), (1, 8), (2, 4)), jnp.float32)
    fidelity = jnp.clip(jnp.exp(math.log(8.0) - 2.7725887 * jax.random.uniform(streams_of[1], (NZ, NY, NX), jnp.float32) ** shard_levels(streams_of[1], (NZ, NY, NX), ((0, 4), (1, 8), (2, 4)), -0.2, 0.2)), 0.5, 8.0)
    primal_u = bell_draw(streams_of[2], (NZ, NY, NX), 1.0, 6.0, ((0, 4), (1, 8), (2, 4)), jnp.float32)
    primal_v = bell_draw(streams_of[3], (3, NZ, NY, NX), 0.3, 2.0, ((1, 4), (2, 8), (3, 4)), jnp.float32)
    dual_p = bell_draw(streams_of[4], (3, NZ, NY, NX), 0.4, 2.5, ((1, 4), (2, 8), (3, 4)), jnp.float32)
    dual_q = bell_draw(streams_of[5], (6, NZ, NY, NX), 0.4, 2.5, ((1, 4), (2, 8), (3, 4)), jnp.float32)
    return {"noisy_image": noisy_image, "fidelity": fidelity, "primal_u": primal_u, "primal_v": primal_v, "dual_p": dual_p, "dual_q": dual_q}


first_alpha = 0.5
second_alpha = 1.0
dual_step = 0.2
primal_step = 0.2
index_pairs = ((0, 0), (1, 1), (2, 2), (0, 1), (0, 2), (1, 2))

def pair_index(left_axis, right_axis):
    for position, entry_pair in enumerate(index_pairs):
        if entry_pair == (left_axis, right_axis) or entry_pair == (right_axis, left_axis):
            return position
    return 0

def shift_next(values, axis_dim):
    extent = values.shape[axis_dim]
    tail_part = lax.slice_in_dim(values, 1, extent, axis=axis_dim)
    zeros_shape = list(values.shape)
    zeros_shape[axis_dim] = 1
    return jnp.concatenate([tail_part, jnp.zeros(zeros_shape, values.dtype)], axis=axis_dim)

def shift_prev(values, axis_dim):
    extent = values.shape[axis_dim]
    head_part = lax.slice_in_dim(values, 0, extent - 1, axis=axis_dim)
    zeros_shape = list(values.shape)
    zeros_shape[axis_dim] = 1
    return jnp.concatenate([jnp.zeros(zeros_shape, values.dtype), head_part], axis=axis_dim)

def edge_masks(extents):
    lower_masks = []
    upper_masks = []
    for component in range(3):
        extent = extents[2 - component]
        places = lax.iota(jnp.int32, extent)
        shape_list = [1, 1, 1, 1]
        shape_list[3 - component] = extent
        upper_masks.append((places < extent - 1).astype(jnp.float32).reshape(shape_list))
        lower_masks.append((places > 0).astype(jnp.float32).reshape(shape_list))
    return (lower_masks, upper_masks)

def q_rows(stacked, column):
    return jnp.stack([stacked[pair_index(row_axis, column)] for row_axis in range(3)], axis=0)

def project(stacked, weights, bound):
    magnitude = jnp.sqrt(lax.optimization_barrier(jnp.sum(weights * stacked * stacked, axis=0, keepdims=True)))
    return stacked / jnp.maximum(1.0, magnitude / bound)

def dual_update(bar_u, bar_v, grad_dual, sym_dual, next_u, prev_v, lower_masks, upper_masks):
    grads = jnp.concatenate([upper_masks[component] * (next_u[component] - bar_u) for component in range(3)], axis=0)
    trial_p = grad_dual + dual_step * (grads - bar_v)
    new_p = project(trial_p, jnp.ones((3, 1, 1, 1), jnp.float32), first_alpha)
    derivs = [lower_masks[component] * (bar_v - prev_v[component]) for component in range(3)]
    sym_parts = []
    for left_axis, right_axis in index_pairs:
        sym_parts.append(0.5 * (derivs[right_axis][left_axis] + derivs[left_axis][right_axis]))
    trial_q = sym_dual + dual_step * jnp.stack(sym_parts, axis=0)
    weights = jnp.array([1.0, 1.0, 1.0, 2.0, 2.0, 2.0], jnp.float32).reshape((6, 1, 1, 1))
    new_q = project(trial_q, weights, second_alpha)
    return (new_p, new_q)

def primal_update(image_u, vector_v, grad_dual, sym_dual, noisy, weight_map, prev_p, next_q, lower_masks, upper_masks):
    divergence = jnp.zeros_like(image_u)
    second_div = jnp.zeros_like(vector_v)
    for component in range(3):
        divergence = divergence + upper_masks[component] * grad_dual[component:component + 1] - prev_p[component]
        second_div = second_div + next_q[component] - lower_masks[component] * q_rows(sym_dual, component)
    new_u = (image_u + primal_step * divergence + primal_step * weight_map * noisy) / (1.0 + primal_step * weight_map)
    new_v = vector_v + primal_step * (grad_dual + second_div)
    return (new_u, new_v)

def reference(noisy_image, fidelity, primal_u, primal_v, dual_p, dual_q):
    noisy = noisy_image[None]
    weight_map = fidelity[None]
    image_u = primal_u[None]
    vector_v = primal_v
    grad_dual = dual_p
    sym_dual = dual_q
    lower_masks, upper_masks = edge_masks(noisy_image.shape)
    bar_u = image_u
    bar_v = vector_v
    for step_index in range(ITERS):
        next_u = [shift_next(bar_u, 3 - component) for component in range(3)]
        prev_v = [shift_prev(bar_v, 3 - component) for component in range(3)]
        grad_dual, sym_dual = dual_update(bar_u, bar_v, grad_dual, sym_dual, next_u, prev_v, lower_masks, upper_masks)
        prev_p = [shift_prev(grad_dual[component:component + 1], 3 - component) for component in range(3)]
        next_q = [shift_next(q_rows(sym_dual, component), 3 - component) for component in range(3)]
        new_u, new_v = primal_update(image_u, vector_v, grad_dual, sym_dual, noisy, weight_map, prev_p, next_q, lower_masks, upper_masks)
        bar_u = 2.0 * new_u - image_u
        bar_v = 2.0 * new_v - vector_v
        image_u = new_u
        vector_v = new_v
    return (image_u[0], vector_v, grad_dual, sym_dual)
```

```python
import functools

import jax
import jax.numpy as jnp
from jax import lax
from jax.experimental import pallas as pl
from jax.experimental.pallas import tpu as pltpu
from jax.sharding import PartitionSpec as P

ITERS = 3
SIGMA = 0.2
TAU = 0.2
ALPHA1 = 0.5
ALPHA0 = 1.0
NZ, NY, NX = 8, 32, 128
TILES = NY // 8
ROWS = NY + 16
PROWS = NY + 8
Q_OF = ((0, 3, 4), (3, 1, 5), (4, 5, 2))
F32 = jnp.float32

(ZUP, ZDN, YUP, YDN, XUP, XDN, XUP_YDN, XDN_YUP, XUP_ZDN, XDN_ZUP, YUP_ZDN, YDN_ZUP,
 PZ, QZ, PY, QY, PX_, QX_) = range(18)
MOVES = {
    ZUP: (0, 0, 1), ZDN: (0, 0, -1), YUP: (0, 1, 0), YDN: (0, -1, 0), XUP: (1, 0, 0), XDN: (-1, 0, 0),
    XUP_YDN: (1, -1, 0), XDN_YUP: (-1, 1, 0), XUP_ZDN: (1, 0, -1), XDN_ZUP: (-1, 0, 1),
    YUP_ZDN: (0, 1, -1), YDN_ZUP: (0, -1, 1),
    PZ: (0, 0, 1), QZ: (0, 0, -1), PY: (0, 1, 0), QY: (0, -1, 0), PX_: (1, 0, 0), QX_: (-1, 0, 0),
}
N_BAR = 12


def p_step(p, here, following, v):
    t = [p[a] + SIGMA * ((following[a] - here) - v[a]) for a in range(3)]
    size = t[0] * t[0] + t[1] * t[1] + t[2] * t[2]
    scale = jnp.minimum(1.0, ALPHA1 * lax.rsqrt(size))
    return [scale * t[a] for a in range(3)]


def q_step(q, v, before):
    d = [[v[a] - before[b][a] for a in range(3)] for b in range(3)]
    s = [q[a] + SIGMA * d[a][a] for a in range(3)]
    s.append(q[3] + (0.5 * SIGMA) * (d[1][0] + d[0][1]))
    s.append(q[4] + (0.5 * SIGMA) * (d[2][0] + d[0][2]))
    s.append(q[5] + (0.5 * SIGMA) * (d[2][1] + d[1][2]))
    size = (s[0] * s[0] + s[1] * s[1] + s[2] * s[2]) + 2.0 * (s[3] * s[3] + s[4] * s[4] + s[5] * s[5])
    scale = jnp.minimum(1.0, ALPHA0 * lax.rsqrt(size))
    return [scale * s[i] for i in range(6)]


def kernel(sizes, f_in, w_in, u_in, v_in, p_in, q_in, u_out, v_out, p_out, q_out,
           bar, barx, uv, p, px, q, qx, fa, wb,
           xlo, xhi, ylo, yhi, e_a, e_b,
           xh_lo, xh_hi, yh_lo, yh_hi, d_xmyp, d_xpym, d_xmzp, d_xpzm, d_ymzp, d_ypzm,
           pyk, qyk, pxk, qxk, ply, quy, plxk, quxk, plx, qux,
           in_sem, out_sem, send_sem, recv_sem):
    names = ("gx", "gy", "gz")
    at = [lax.axis_index(n) for n in names]
    up = [at[i] < sizes[i] - 1 for i in range(3)]
    down = [at[i] > 0 for i in range(3)]

    def exists(move):
        flag = None
        for i in range(3):
            if move[i]:
                one = up[i] if move[i] > 0 else down[i]
                flag = one if flag is None else jnp.logical_and(flag, one)
        return flag

    def device(move):
        return {names[i]: at[i] + move[i] for i in range(3) if move[i]}

    def opposite(move):
        return tuple(-m for m in move)

    loads = [
        pltpu.make_async_copy(u_in, bar.at[0, 0, 1 : NZ + 1, 8 : 8 + NY, :], in_sem.at[0]),
        pltpu.make_async_copy(v_in, bar.at[0, 1:4, 1 : NZ + 1, 8 : 8 + NY, :], in_sem.at[1]),
        pltpu.make_async_copy(p_in, p.at[:, 1 : NZ + 1, 8 : 8 + NY, :], in_sem.at[2]),
        pltpu.make_async_copy(q_in, q.at[:, 0:NZ, 0:NY, :], in_sem.at[3]),
        pltpu.make_async_copy(f_in, fa, in_sem.at[4]),
        pltpu.make_async_copy(w_in, wb, in_sem.at[5]),
    ]
    for c in loads:
        c.start()

    barrier = pltpu.get_barrier_semaphore()
    arrivals = jnp.int32(0)
    for m in range(N_BAR):
        move = MOVES[m]
        arrivals = arrivals + exists(move).astype(jnp.int32)

        @pl.when(exists(move))
        def _():
            pl.semaphore_signal(
                barrier, inc=1, device_id=device(move), device_id_type=pl.DeviceIdType.MESH
            )

    def ends(m, r):
        if m == ZUP:
            return bar.at[r, :, NZ, 8 : 8 + NY, :], bar.at[r, :, 0, 8 : 8 + NY, :]
        if m == ZDN:
            return bar.at[r, :, 1, 8 : 8 + NY, :], bar.at[r, :, NZ + 1, 8 : 8 + NY, :]
        if m == PZ:
            return p_in.at[:, NZ - 1, :, :], p.at[:, 0, 8 : 8 + NY, :]
        if m == QZ:
            return q_in.at[:, 0, :, :], q.at[:, NZ, 0:NY, :]
        if m in (PY, QY, PX_, QX_):
            return {PY: (pyk, ply), QY: (qyk, quy), PX_: (pxk, plxk), QX_: (qxk, quxk)}[m]
        src, dst = {
            YUP: (yhi, yh_lo), YDN: (ylo, yh_hi), XUP: (xhi, xh_lo), XDN: (xlo, xh_hi),
            XUP_YDN: (xhi, d_xmyp), XDN_YUP: (xlo, d_xpym),
            XUP_ZDN: (xhi, d_xmzp), XDN_ZUP: (xlo, d_xpzm),
            YUP_ZDN: (e_a, d_ymzp), YDN_ZUP: (e_b, d_ypzm),
        }[m]
        return src.at[r], dst.at[r]

    def message(m, r):
        src, dst = ends(m, r)
        return pltpu.make_async_remote_copy(
            src_ref=src, dst_ref=dst, send_sem=send_sem.at[r, m], recv_sem=recv_sem.at[r, m],
            device_id=device(MOVES[m]), device_id_type=pl.DeviceIdType.MESH,
        )

    def messages(r):
        return range(18) if r == 0 else range(N_BAR)

    def send(r):
        for m in messages(r):
            @pl.when(exists(MOVES[m]))
            def _():
                message(m, r).start()

    def receive(r):
        for m in messages(r):
            @pl.when(exists(opposite(MOVES[m])))
            def _():
                message(m, r).wait_recv()

    lane = lax.broadcasted_iota(jnp.int32, (8, 128), 1)
    sub = lax.broadcasted_iota(jnp.int32, (8, 128), 0)

    def lanes(x, by):
        by = by % 128
        return x if isinstance(by, int) and by == 0 else pltpu.roll(x, by, 1)

    def subs(x, by):
        return pltpu.roll(x, by % 8, 0)

    first = lane == 0
    last = lane == 127

    def flagged(cond, x, other):
        return jnp.where(cond, x, other)

    def pack_pair(z, t, values, low, high):
        for f, x in enumerate(values):
            s = f * 32 + z * 4 + t
            rolled = pltpu.roll(x, s, 1)
            low = jnp.where(lane == s, rolled, low)
            high = jnp.where(lane == lax.rem(s + 127, 128), rolled, high)
        return low, high

    zero = jnp.zeros((8, 128), F32)

    def edges_out(r, z, t, values):
        for f, x in enumerate(values):
            if t == 0:
                ylo[r, f, pl.ds(z, 1), :] = x[0:1, :]
            if t == TILES - 1:
                yhi[r, f, pl.ds(z, 1), :] = x[7:8, :]

    def lines_out(r):
        for f in range(4):
            e_a[r, f : f + 1, :] = yhi[r, f, 0:1, :]
            e_b[r, f : f + 1, :] = ylo[r, f, NZ - 1 : NZ, :]

    def rolled_out(z, t, values):
        rows = pl.ds(8 * t, 8)
        barx[0, z, rows, :] = lanes(values[0], -1)
        for a in range(3):
            barx[1 + a, z, rows, :] = lanes(values[1 + a], 1)

    loads[0].wait()
    loads[1].wait()

    def first_pack(z, carry):
        low, high = carry
        for t in range(TILES):
            values = [bar[0, f, z + 1, 8 + 8 * t : 16 + 8 * t, :] for f in range(4)]
            low, high = pack_pair(z, t, values, low, high)
            edges_out(0, z, t, values)
            rolled_out(z, t, values)
        return low, high

    low, high = lax.fori_loop(0, NZ, first_pack, (zero, zero))
    xlo[0] = low
    xhi[0] = lanes(high, 1)
    lines_out(0)
    loads[2].wait()
    loads[3].wait()

    def pq_pack(z, carry):
        ph, q1, q2 = carry
        for t in range(TILES):
            for a in range(3):
                x = p[a, z + 1, 8 + 8 * t : 16 + 8 * t, :]
                s = a * 32 + z * 4 + t
                ph = jnp.where(lane == s, pltpu.roll(x, s + 1, 1), ph)
                if t == TILES - 1:
                    pyk[a, pl.ds(z, 1), :] = x[7:8, :]
            for i in range(6):
                x = q[i, z, 8 * t : 8 * t + 8, :]
                s = (i % 3) * 32 + z * 4 + t
                rolled = pltpu.roll(x, s, 1)
                if i < 3:
                    q1 = jnp.where(lane == s, rolled, q1)
                else:
                    q2 = jnp.where(lane == s, rolled, q2)
                if t == 0:
                    qyk[i, pl.ds(z, 1), :] = x[0:1, :]
        return ph, q1, q2

    ph, q1, q2 = lax.fori_loop(0, NZ, pq_pack, (zero, zero, zero))
    pxk[...] = ph
    qxk[0] = q1
    qxk[1] = q2

    pl.semaphore_wait(barrier, arrivals)
    send(0)

    loads[4].wait()
    loads[5].wait()

    def weights(z, carry):
        for t in range(TILES):
            rows = pl.ds(8 * t, 8)
            tw = TAU * wb[z, rows, :]
            fa[z, rows, :] = tw * fa[z, rows, :]
            wb[z, rows, :] = 1.0 / (1.0 + tw)
        return carry

    lax.fori_loop(0, NZ, weights, 0)

    def clamp(r):
        @pl.when(jnp.logical_not(up[0]))
        def _():
            xh_hi[r] = xhi[r]

        @pl.when(jnp.logical_not(down[0]))
        def _():
            xh_lo[r] = xlo[r]

        @pl.when(jnp.logical_not(up[1]))
        def _():
            yh_hi[r] = yhi[r]

        @pl.when(jnp.logical_not(down[1]))
        def _():
            yh_lo[r] = ylo[r]

        @pl.when(jnp.logical_not(up[2]))
        def _():
            bar[r, :, NZ + 1, 8 : 8 + NY, :] = bar[r, :, NZ, 8 : 8 + NY, :]

        @pl.when(jnp.logical_not(down[2]))
        def _():
            bar[r, :, 0, 8 : 8 + NY, :] = bar[r, :, 1, 8 : 8 + NY, :]

    mask_px = jnp.where(jnp.logical_and(last, jnp.logical_not(up[0])), 0.0, 1.0).astype(F32)
    mask_qx = jnp.where(jnp.logical_and(first, jnp.logical_not(down[0])), 0.0, 1.0).astype(F32)
    mask_py = jnp.where(jnp.logical_and(sub == 7, jnp.logical_not(up[1])), 0.0, 1.0).astype(F32)
    mask_qy = jnp.where(jnp.logical_and(sub == 0, jnp.logical_not(down[1])), 0.0, 1.0).astype(F32)

    in32 = lax.rem(lane, 32)
    in4 = lax.rem(lane, 4)

    def layers(r):
        low = xh_lo[r]
        a = subs(low, -1)
        edge = lanes(subs(d_xmyp[r], -1), 3)
        ny = jnp.where(sub < 7, a, jnp.where(in4 < 3, lanes(a, -1), flagged(up[1], edge, low)))
        nz = jnp.where(in32 < 28, lanes(low, -4), flagged(up[2], lanes(d_xmzp[r], 28), low))
        new = p_step([plx[c] for c in range(3)], low, [xlo[r], ny, nz],
                     [lanes(low, -32 * (1 + c)) for c in range(3)])
        for c in range(3):
            plx[c] = new[c]
        below_x = flagged(down[0], new[0], zero)

        high = xh_hi[r]
        a = subs(high, 1)
        edge = lanes(subs(d_xpym[r], 1), -3)
        py_ = jnp.where(sub > 0, a, jnp.where(in4 > 0, lanes(a, 1), flagged(down[1], edge, high)))
        pz_ = jnp.where(in32 >= 4, lanes(high, 4), flagged(down[2], lanes(d_xpzm[r], -28), high))
        own = xhi[r]

        def split(x):
            return [lanes(x, -32 * (1 + c)) for c in range(3)]

        new = q_step([qux[i] for i in range(6)], split(high), [split(own), split(py_), split(pz_)])
        for i in range(6):
            qux[i] = new[i]
        above_x = [flagged(up[0], new[i], zero) for i in Q_OF[0]]

        here = yh_lo[r, 0]
        row = jnp.broadcast_to(d_xpym[r, 7:8, :], (8, 128))
        col = jnp.sum(jnp.where(lane == 4 * sub + 3, row, 0.0), axis=1, keepdims=True)
        nx = jnp.where(lane < 127, lanes(here, -1), flagged(up[0], jnp.broadcast_to(col, (8, 128)), here))
        line = jnp.broadcast_to(d_ymzp[r, 0:1, :], (8, 128))
        nz = jnp.where(sub < 7, subs(here, -1), flagged(up[2], line, here))
        new = p_step([ply[c] for c in range(3)], here, [nx, ylo[r, 0], nz],
                     [yh_lo[r, 1 + c] for c in range(3)])
        for c in range(3):
            ply[c] = new[c]
        below_y = flagged(down[1], new[1], zero)
        for z in range(NZ):
            p[1, z + 1, 7:8, :] = below_y[z : z + 1, :]

        v = [yh_hi[r, 1 + c] for c in range(3)]
        row = jnp.broadcast_to(d_xmyp[r, 0:1, :], (8, 128))
        bx, bz = [], []
        for c in range(3):
            col = jnp.sum(jnp.where(lane == 4 * sub + 32 * (1 + c), row, 0.0), axis=1, keepdims=True)
            bx.append(jnp.where(lane > 0, lanes(v[c], 1),
                                flagged(down[0], jnp.broadcast_to(col, (8, 128)), v[c])))
            line = jnp.broadcast_to(d_ypzm[r, 1 + c : 2 + c, :], (8, 128))
            bz.append(jnp.where(sub > 0, subs(v[c], 1), flagged(down[2], line, v[c])))
        new = q_step([quy[i] for i in range(6)], v, [bx, [yhi[r, 1 + c] for c in range(3)], bz])
        for i in range(6):
            quy[i] = new[i]
        for i in Q_OF[1]:
            above_y = flagged(up[1], new[i], zero)
            for z in range(NZ):
                q[i, z, NY : NY + 1, :] = above_y[z : z + 1, :]

        bar[r, 0, 0, 8 + NY : 9 + NY, :] = flagged(up[1], d_ypzm[r, 0:1, :], bar[r, 0, 0, 7 + NY : 8 + NY, :])
        for c in range(3):
            bar[r, 1 + c, NZ + 1, 7:8, :] = flagged(down[1], d_ymzp[r, 1 + c : 2 + c, :],
                                                    bar[r, 1 + c, NZ + 1, 8:9, :])
        dn, du = d_xpzm[r], d_xmzp[r]
        for t in range(TILES):
            rows = slice(8 + 8 * t, 16 + 8 * t)
            here = bar[r, 0, 0, rows, :]
            nx = jnp.where(lane < 127, lanes(here, -1), flagged(up[0], lanes(dn, 127 - 28 - t), here))
            new = p_step([p[c, 0, rows, :] for c in range(3)], here,
                         [nx, bar[r, 0, 0, 9 + 8 * t : 17 + 8 * t, :], bar[r, 0, 1, rows, :]],
                         [bar[r, 1 + c, 0, rows, :] for c in range(3)])
            new[2] = flagged(down[2], new[2], zero)
            for c in range(3):
                p[c, 0, rows, :] = new[c]

            v = [bar[r, 1 + c, NZ + 1, rows, :] for c in range(3)]
            bx = [jnp.where(lane > 0, lanes(v[c], 1), flagged(down[0], lanes(du, -32 * (1 + c) - t), v[c]))
                  for c in range(3)]
            new = q_step([q[i, NZ, 8 * t : 8 * t + 8, :] for i in range(6)], v,
                         [bx, [bar[r, 1 + c, NZ + 1, 7 + 8 * t : 15 + 8 * t, :] for c in range(3)],
                          [bar[r, 1 + c, NZ, rows, :] for c in range(3)]])
            for i in range(6):
                value = flagged(up[2], new[i], zero) if i in Q_OF[2] else new[i]
                q[i, NZ, 8 * t : 8 * t + 8, :] = value
        return below_x, above_x

    def patch(r):
        high = xh_hi[r]
        low = xh_lo[r]
        for z in range(NZ):
            bar[r, 0, z + 1, 8 + NY : 9 + NY, :] = yh_hi[r, 0, z : z + 1, :]
            for c in range(3):
                bar[r, 1 + c, z + 1, 7:8, :] = yh_lo[r, 1 + c, z : z + 1, :]

        def body(z, carry):
            for t in range(TILES):
                rows = pl.ds(8 * t, 8)
                s = z * 4 + t
                old = barx[0, z, rows, :]
                barx[0, z, rows, :] = jnp.where(last, pltpu.roll(high, 127 - s, 1), old)
                for c in range(3):
                    old = barx[1 + c, z, rows, :]
                    barx[1 + c, z, rows, :] = jnp.where(
                        first, pltpu.roll(low, lax.rem(256 - 32 * (1 + c) - s, 128), 1), old)
            return carry

        lax.fori_loop(0, NZ, body, 0)

    def patch_pq(below_x, above_x):
        def body(z, carry):
            for t in range(TILES):
                rows = pl.ds(8 * t, 8)
                s = z * 4 + t
                px[z, rows, :] = jnp.where(first, pltpu.roll(below_x, lax.rem(128 - s, 128), 1), px[z, rows, :])
                for j in range(3):
                    qx[j, z, rows, :] = jnp.where(last, pltpu.roll(above_x[j], 127 - s, 1), qx[j, z, rows, :])
            return carry

        lax.fori_loop(0, NZ, body, 0)

    def dual(r):
        def body(z, carry):
            for t in range(TILES):
                rows = slice(8 + 8 * t, 16 + 8 * t)
                mine = slice(8 * t, 8 * t + 8)
                here = bar[r, 0, z + 1, rows, :]
                v = [bar[r, 1 + c, z + 1, rows, :] for c in range(3)]
                new = p_step([p[c, z + 1, rows, :] for c in range(3)], here,
                             [barx[0, z, mine, :], bar[r, 0, z + 1, 9 + 8 * t : 17 + 8 * t, :],
                              bar[r, 0, z + 2, rows, :]], v)
                for c in range(3):
                    p[c, z + 1, rows, :] = new[c]
                px[z, mine, :] = lanes(new[0], 1)
                new = q_step([q[i, z, mine, :] for i in range(6)], v,
                             [[barx[1 + c, z, mine, :] for c in range(3)],
                              [bar[r, 1 + c, z + 1, 7 + 8 * t : 15 + 8 * t, :] for c in range(3)],
                              [bar[r, 1 + c, z, rows, :] for c in range(3)]])
                for i in range(6):
                    q[i, z, mine, :] = new[i]
                for j, i in enumerate(Q_OF[0]):
                    qx[j, z, mine, :] = lanes(new[i], -1)
            return carry

        lax.fori_loop(0, NZ, body, 0)

    def primal(r):
        final = r == ITERS - 1

        def body(z, carry):
            low, high = carry
            mask_pz = jnp.where(jnp.logical_and(z == NZ - 1, jnp.logical_not(up[2])), 0.0, 1.0).astype(F32)
            mask_qz = jnp.where(jnp.logical_and(z == 0, jnp.logical_not(down[2])), 0.0, 1.0).astype(F32)
            for t in range(TILES):
                rows = slice(8 + 8 * t, 16 + 8 * t)
                mine = slice(8 * t, 8 * t + 8)
                pv = [p[c, z + 1, rows, :] for c in range(3)]
                div = mask_px * pv[0] - px[z, mine, :]
                own = mask_py * pv[1] if t == TILES - 1 else pv[1]
                div = div + own - p[1, z + 1, 7 + 8 * t : 15 + 8 * t, :]
                div = div + mask_pz * pv[2] - p[2, z, rows, :]
                if r == 0:
                    old = [bar[0, f, z + 1, rows, :] for f in range(4)]
                else:
                    old = [uv[f, z, mine, :] for f in range(4)]
                new = [(old[0] + TAU * div + fa[z, mine, :]) * wb[z, mine, :]]
                qv = [q[i, z, mine, :] for i in range(6)]
                for a in range(3):
                    ix, iy, iz = Q_OF[a]
                    total = qx[a, z, mine, :] - mask_qx * qv[ix]
                    own = mask_qy * qv[iy] if t == 0 else qv[iy]
                    total = total + q[iy, z, 1 + 8 * t : 9 + 8 * t, :] - own
                    total = total + q[iz, z + 1, mine, :] - mask_qz * qv[iz]
                    new.append(old[1 + a] + TAU * (pv[a] + total))
                for f in range(4):
                    uv[f, z, mine, :] = new[f]
                if not final:
                    values = [2.0 * new[f] - old[f] for f in range(4)]
                    for f in range(4):
                        bar[r + 1, f, z + 1, rows, :] = values[f]
                    low, high = pack_pair(z, t, values, low, high)
                    edges_out(r + 1, z, t, values)
                    rolled_out(z, t, values)
            return low, high

        low, high = lax.fori_loop(0, NZ, body, (zero, zero))
        if not final:
            xlo[r + 1] = low
            xhi[r + 1] = lanes(high, 1)
            lines_out(r + 1)

    stores = [
        pltpu.make_async_copy(p.at[:, 1 : NZ + 1, 8 : 8 + NY, :], p_out, out_sem.at[0]),
        pltpu.make_async_copy(q.at[:, 0:NZ, 0:NY, :], q_out, out_sem.at[1]),
        pltpu.make_async_copy(uv.at[0], u_out, out_sem.at[2]),
        pltpu.make_async_copy(uv.at[1:4], v_out, out_sem.at[3]),
    ]
    for r in range(ITERS):
        receive(r)
        clamp(r)
        if r == 0:
            packed = plxk[...]
            for c in range(3):
                plx[c] = lanes(packed, -32 * c)
            for i in range(6):
                qux[i] = lanes(quxk[i // 3], -32 * (i % 3))
        patch(r)
        below_x, above_x = layers(r)
        dual(r)
        patch_pq(below_x, above_x)
        if r == ITERS - 1:
            stores[0].start()
            stores[1].start()
        primal(r)
        if r < ITERS - 1:
            send(r + 1)
    stores[2].start()
    stores[3].start()
    for r in range(ITERS):
        for m in messages(r):
            @pl.when(exists(MOVES[m]))
            def _():
                message(m, r).wait_send()
    for c in stores:
        c.wait()


def per_device(sizes, *arrays):
    anywhere = pl.BlockSpec(memory_space=pl.ANY)
    tile = (8, 128)

    def vmem(*shape):
        return pltpu.VMEM(shape, F32)

    return pl.pallas_call(
        functools.partial(kernel, sizes),
        out_shape=tuple(jax.ShapeDtypeStruct(s, F32) for s in
                        ((NZ, NY, NX), (3, NZ, NY, NX), (3, NZ, NY, NX), (6, NZ, NY, NX))),
        in_specs=[anywhere] * 6,
        out_specs=(anywhere,) * 4,
        scratch_shapes=[
            vmem(ITERS, 4, NZ + 2, ROWS, NX),
            vmem(4, NZ, NY, NX),
            vmem(4, NZ, NY, NX),
            vmem(3, NZ + 1, PROWS, NX),
            vmem(NZ, NY, NX),
            vmem(6, NZ + 1, PROWS, NX),
            vmem(3, NZ, NY, NX),
            vmem(NZ, NY, NX),
            vmem(NZ, NY, NX),
            vmem(ITERS, *tile), vmem(ITERS, *tile),
            vmem(ITERS, 4, *tile), vmem(ITERS, 4, *tile),
            vmem(ITERS, 4, 128), vmem(ITERS, 4, 128),
            vmem(ITERS, *tile), vmem(ITERS, *tile),
            vmem(ITERS, 4, *tile), vmem(ITERS, 4, *tile),
            vmem(ITERS, *tile), vmem(ITERS, *tile), vmem(ITERS, *tile), vmem(ITERS, *tile),
            vmem(ITERS, 4, 128), vmem(ITERS, 4, 128),
            vmem(3, *tile), vmem(6, *tile), vmem(*tile), vmem(2, *tile),
            vmem(3, *tile), vmem(6, *tile), vmem(*tile), vmem(2, *tile),
            vmem(3, *tile), vmem(6, *tile),
            pltpu.SemaphoreType.DMA((6,)),
            pltpu.SemaphoreType.DMA((4,)),
            pltpu.SemaphoreType.DMA((ITERS, 18)),
            pltpu.SemaphoreType.DMA((ITERS, 18)),
        ],
        compiler_params=pltpu.CompilerParams(collective_id=0, has_side_effects=True),
        name="tgv",
    )(*arrays)


def solution(mesh):
    sizes = tuple(mesh.shape[n] for n in ("gx", "gy", "gz"))
    scalar = P("gz", "gy", "gx")
    stack = P(None, "gz", "gy", "gx")
    return jax.shard_map(
        functools.partial(per_device, sizes), mesh=mesh,
        in_specs=(scalar, scalar, scalar, stack, stack, stack),
        out_specs=(scalar, stack, stack, stack), check_vma=False,
    )
```

```python
import functools

import jax
import jax.numpy as jnp
from jax import lax
from jax.experimental import pallas as pl
from jax.experimental.pallas import tpu as pltpu
from jax.sharding import PartitionSpec as P

ITERS = 3
SIGMA = 0.2
TAU = 0.2
ALPHA1 = 0.5
ALPHA0 = 1.0
NZ, NY, NX = 8, 32, 128
TILES = NY // 8
ROWS = NY + 16
PROWS = NY + 8
Q_OF = ((0, 3, 4), (3, 1, 5), (4, 5, 2))
F32 = jnp.float32
NAMES = ("gx", "gy", "gz")

(ZUP, ZDN, YUP, YDN, XUP, XDN, XUP_YDN, XDN_YUP, XUP_ZDN, XDN_ZUP, YUP_ZDN, YDN_ZUP,
 PZ, QZ, PY, QY, PX_, QX_) = range(18)
MOVES = {
    ZUP: (0, 0, 1), ZDN: (0, 0, -1), YUP: (0, 1, 0), YDN: (0, -1, 0), XUP: (1, 0, 0), XDN: (-1, 0, 0),
    XUP_YDN: (1, -1, 0), XDN_YUP: (-1, 1, 0), XUP_ZDN: (1, 0, -1), XDN_ZUP: (-1, 0, 1),
    YUP_ZDN: (0, 1, -1), YDN_ZUP: (0, -1, 1),
    PZ: (0, 0, 1), QZ: (0, 0, -1), PY: (0, 1, 0), QY: (0, -1, 0), PX_: (1, 0, 0), QX_: (-1, 0, 0),
}
N_BAR = 12
FAR = (XUP_YDN, XDN_YUP, YUP, YDN, YUP_ZDN, YDN_ZUP)
NEAR = (ZDN, ZUP, XUP, XDN, XUP_ZDN, XDN_ZUP)
FAR0 = FAR + (QY, PY)
NEAR0 = NEAR + (QZ, PZ, PX_, QX_)
INNER = tuple(range(1, TILES - 1))
OUTER = (0, TILES - 1)
EVERY = tuple(range(TILES))


def p_step(p, here, following, v):
    t = [p[a] + SIGMA * ((following[a] - here) - v[a]) for a in range(3)]
    size = t[0] * t[0] + t[1] * t[1] + t[2] * t[2]
    scale = jnp.minimum(1.0, ALPHA1 * lax.rsqrt(size))
    return [scale * t[a] for a in range(3)]


def q_step(q, v, before):
    d = [[v[a] - before[b][a] for a in range(3)] for b in range(3)]
    s = [q[a] + SIGMA * d[a][a] for a in range(3)]
    s.append(q[3] + (0.5 * SIGMA) * (d[1][0] + d[0][1]))
    s.append(q[4] + (0.5 * SIGMA) * (d[2][0] + d[0][2]))
    s.append(q[5] + (0.5 * SIGMA) * (d[2][1] + d[1][2]))
    size = (s[0] * s[0] + s[1] * s[1] + s[2] * s[2]) + 2.0 * (s[3] * s[3] + s[4] * s[4] + s[5] * s[5])
    scale = jnp.minimum(1.0, ALPHA0 * lax.rsqrt(size))
    return [scale * s[i] for i in range(6)]


def lanes(x, by):
    return x if by % 128 == 0 else pltpu.roll(x, by % 128, 1)


def subs(x, by):
    return pltpu.roll(x, by % 8, 0)


def tile_iota(axis):
    return lax.broadcasted_iota(jnp.int32, (8, 128), axis)


def place(sizes):
    at = [lax.axis_index(n) for n in NAMES]
    return at, [at[i] < sizes[i] - 1 for i in range(3)], [at[i] > 0 for i in range(3)]


def primal_tile(z, t, masks, p, q, old, weight, below_x, above_x):
    first, last = masks[6], masks[7]
    rows = slice(8 + 8 * t, 16 + 8 * t)
    mine = slice(8 * t, 8 * t + 8)
    s = z * TILES + t
    pv = [p[c, z + 1, rows, :] for c in range(3)]
    div = masks[0] * pv[0] - jnp.where(first, lanes(below_x, -2 * s), lanes(pv[0], 1))
    div = div + ((masks[2] * pv[1] if t == TILES - 1 else pv[1]) - p[1, z + 1, 7 + 8 * t : 15 + 8 * t, :])
    div = div + ((masks[4] * pv[2] if z == NZ - 1 else pv[2]) - p[2, z, rows, :])
    fw, inverse = weight
    new = [(old[0] + TAU * div + fw) * inverse]
    bars = [2.0 * new[0] - old[0]]
    qv = [q[i, z, mine, :] for i in range(6)]
    qn = [jnp.where(last, lanes(above_x[j], 127 - 2 * s), lanes(qv[i], -1)) for j, i in enumerate(Q_OF[0])]
    for a in range(3):
        ix, iy, iz = Q_OF[a]
        total = pv[a] + (qn[a] - masks[1] * qv[ix])
        total = total + (q[iy, z, 1 + 8 * t : 9 + 8 * t, :] - (masks[3] * qv[iy] if t == 0 else qv[iy]))
        total = total + (q[iz, z + 1, mine, :] - (masks[5] * qv[iz] if z == 0 else qv[iz]))
        step = TAU * total
        new.append(old[1 + a] + step)
        bars.append(new[1 + a] + step)
    return new, bars


def edge_masks(up, down):
    lane, sub = tile_iota(1), tile_iota(0)
    first, last = lane == 0, lane == 127

    def at(where, inside):
        return jnp.where(jnp.logical_and(where, jnp.logical_not(inside)), 0.0, 1.0).astype(F32)

    return (at(last, up[0]), at(first, down[0]), at(sub == 7, up[1]), at(sub == 0, down[1]),
            jnp.where(up[2], 1.0, 0.0).astype(F32), jnp.where(down[2], 1.0, 0.0).astype(F32), first, last)


def exchange_kernel(sizes, f_in, w_in, u_in, v_in, p_in, q_in,
                    uv, p, q, fa, wb, cols,
                    bar0, bar1, bar2, xe, xey, xh_lo, xh_hi, d_xmyp, d_xpym, d_xmzp, d_xpzm,
                    pxk, qxk, plxk, quxk, plx, qux,
                    in_sem, send_sem, recv_sem):
    at, up, down = place(sizes)
    bars = (bar0, bar1, bar2)

    def exists(move):
        flag = None
        for i in range(3):
            if move[i]:
                one = up[i] if move[i] > 0 else down[i]
                flag = one if flag is None else jnp.logical_and(flag, one)
        return flag

    def device(move):
        return {NAMES[i]: at[i] + move[i] for i in range(3) if move[i]}

    def opposite(move):
        return tuple(-m for m in move)

    loads = [
        pltpu.make_async_copy(u_in, bar0.at[0, 1 : NZ + 1, 8 : 8 + NY, :], in_sem.at[0]),
        pltpu.make_async_copy(v_in, bar0.at[1:4, 1 : NZ + 1, 8 : 8 + NY, :], in_sem.at[1]),
        pltpu.make_async_copy(p_in, p.at[:, 1 : NZ + 1, 8 : 8 + NY, :], in_sem.at[2]),
        pltpu.make_async_copy(q_in, q.at[:, 0:NZ, 0:NY, :], in_sem.at[3]),
        pltpu.make_async_copy(f_in, fa, in_sem.at[4]),
        pltpu.make_async_copy(w_in, wb, in_sem.at[5]),
    ]
    barrier = pltpu.get_barrier_semaphore()
    arrivals = jnp.int32(0)
    for m in FAR + NEAR:
        move = MOVES[m]
        arrivals = arrivals + exists(move).astype(jnp.int32)

        @pl.when(exists(move))
        def _():
            pl.semaphore_signal(
                barrier, inc=1, device_id=device(move), device_id_type=pl.DeviceIdType.MESH
            )

    for c in loads:
        c.start()

    def ends(m, r):
        bar = bars[r]
        inner = slice(1, NZ + 1)
        if m == ZUP:
            return bar.at[:, NZ, 8 : 8 + NY, :], bar.at[:, 0, 8 : 8 + NY, :]
        if m == ZDN:
            return bar.at[:, 1, 8 : 8 + NY, :], bar.at[:, NZ + 1, 8 : 8 + NY, :]
        if m == YUP:
            return bar.at[:, 1 : NZ + 1, 7 + NY, :], bar.at[:, 1 : NZ + 1, 7, :]
        if m == YDN:
            return bar.at[:, 1 : NZ + 1, 8, :], bar.at[:, 1 : NZ + 1, 8 + NY, :]
        if m == YUP_ZDN:
            return bar.at[:, 1, 7 + NY, :], bar.at[:, NZ + 1, 7, :]
        if m == YDN_ZUP:
            return bar.at[:, NZ, 8, :], bar.at[:, 0, 8 + NY, :]
        if m == PZ:
            return p_in.at[:, NZ - 1, :, :], p.at[:, 0, 8 : 8 + NY, :]
        if m == QZ:
            return q_in.at[:, 0, :, :], q.at[:, NZ, 0:NY, :]
        if m == PY:
            return p_in.at[:, :, NY - 1, :], p.at[:, 1 : NZ + 1, 7, :]
        if m == QY:
            return q_in.at[:, :, 0, :], q.at[:, 0:NZ, NY, :]
        if m == PX_:
            return pxk, plxk
        if m == QX_:
            return qxk, quxk
        src, dst = {
            XUP: (xe, xh_lo), XDN: (xe, xh_hi), XUP_YDN: (xey, d_xmyp), XDN_YUP: (xey, d_xpym),
            XUP_ZDN: (xe, d_xmzp), XDN_ZUP: (xe, d_xpzm),
        }[m]
        return src.at[r], dst.at[r]

    def message(m, r):
        src, dst = ends(m, r)
        return pltpu.make_async_remote_copy(
            src_ref=src, dst_ref=dst, send_sem=send_sem.at[r, m], recv_sem=recv_sem.at[r, m],
            device_id=device(MOVES[m]), device_id_type=pl.DeviceIdType.MESH,
        )

    def send(r, which):
        for m in which:
            @pl.when(exists(MOVES[m]))
            def _():
                message(m, r).start()

    def receive(r, which):
        for m in which:
            @pl.when(exists(opposite(MOVES[m])))
            def _():
                message(m, r).wait_recv()

    lane, sub = tile_iota(1), tile_iota(0)
    first, last = lane == 0, lane == 127
    edge = jnp.logical_or(first, last)
    zero = jnp.zeros((8, 128), F32)
    masks = edge_masks(up, down)

    def pack_into(acc, z, t, values, mask, by):
        for f, x in enumerate(values):
            acc[f // 2] = acc[f // 2] + lanes(jnp.where(mask, x, 0.0), (f % 2) * 64 + 2 * (z * TILES + t) + by)

    loads[0].wait()
    loads[1].wait()
    acc = [zero, zero]
    for t in OUTER + INNER:
        for z in range(NZ):
            pack_into(acc, z, t, [bar0[f, z + 1, 8 + 8 * t : 16 + 8 * t, :] for f in range(4)], edge, 0)
        if t == OUTER[-1]:
            for h in range(2):
                xey[0, h] = acc[h]
    for h in range(2):
        xe[0, h] = acc[h]
    loads[2].wait()
    loads[3].wait()
    accp, accq = [zero, zero], [zero, zero, zero]
    for t in EVERY:
        for z in range(NZ):
            pack_into(accp, z, t, [p[a, z + 1, 8 + 8 * t : 16 + 8 * t, :] for a in range(3)], last, 1)
            pack_into(accq, z, t, [q[i, z, 8 * t : 8 * t + 8, :] for i in range(6)], first, 0)
    for h in range(2):
        pxk[h] = accp[h]
    for h in range(3):
        qxk[h] = accq[h]

    pl.semaphore_wait(barrier, arrivals)
    send(0, FAR0)
    send(0, NEAR0)

    loads[4].wait()
    loads[5].wait()
    for z in range(NZ):
        for t in EVERY:
            rows = slice(8 * t, 8 * t + 8)
            tw = TAU * wb[z, rows, :]
            fa[z, rows, :] = tw * fa[z, rows, :]
            wb[z, rows, :] = 1.0 / (1.0 + tw)

    def split(x):
        return [x[0], lanes(x[0], 64), x[1], lanes(x[1], 64)]

    def clamp_near(r):
        bar = bars[r]

        @pl.when(jnp.logical_not(up[0]))
        def _():
            for h in range(2):
                xh_hi[r, h] = lanes(xe[r, h], 1)

        @pl.when(jnp.logical_not(down[0]))
        def _():
            for h in range(2):
                xh_lo[r, h] = lanes(xe[r, h], -1)

        @pl.when(jnp.logical_not(up[2]))
        def _():
            bar[:, NZ + 1, 8 : 8 + NY, :] = bar[:, NZ, 8 : 8 + NY, :]

        @pl.when(jnp.logical_not(down[2]))
        def _():
            bar[:, 0, 8 : 8 + NY, :] = bar[:, 1, 8 : 8 + NY, :]

    def clamp_far(r):
        bar = bars[r]

        @pl.when(jnp.logical_not(up[2]))
        def _():
            for f in range(4):
                bar[f, NZ + 1, 7:8, :] = bar[f, NZ, 7:8, :]

        @pl.when(jnp.logical_not(down[2]))
        def _():
            for f in range(4):
                bar[f, 0, 8 + NY : 9 + NY, :] = bar[f, 1, 8 + NY : 9 + NY, :]

        @pl.when(jnp.logical_not(up[1]))
        def _():
            for f in range(4):
                bar[f, 0, 8 + NY : 9 + NY, :] = bar[f, 0, 7 + NY : 8 + NY, :]
                bar[f, 1 : NZ + 1, 8 + NY, :] = bar[f, 1 : NZ + 1, 7 + NY, :]

        @pl.when(jnp.logical_not(down[1]))
        def _():
            for f in range(4):
                bar[f, NZ + 1, 7:8, :] = bar[f, NZ + 1, 8:9, :]
                bar[f, 1 : NZ + 1, 7, :] = bar[f, 1 : NZ + 1, 8, :]

    in64 = lax.rem(lane, 64)
    in8 = lax.rem(lane, 8)

    def layers(r):
        bar = bars[r]
        own = [xe[r, h] for h in range(2)]
        own_high = [lanes(x, 1) for x in own]
        low = [lanes(xh_lo[r, h], 1) for h in range(2)]
        here = low[0]
        a = subs(here, -1)
        corner = lanes(subs(d_xmyp[r, 0], -1), 7)
        ny = jnp.where(sub < 7, a, jnp.where(in8 < 6, lanes(a, -2), jnp.where(up[1], corner, here)))
        nz = jnp.where(in64 < 56, lanes(here, -8), jnp.where(up[2], lanes(d_xmzp[r, 0], 57), here))
        new = p_step([plx[c] for c in range(3)], here, [own[0], ny, nz], split(low)[1:])
        for c in range(3):
            plx[c] = new[c]
        below_x = jnp.where(down[0], new[0], zero)

        high = [xh_hi[r, h] for h in range(2)]
        py_, pz_ = [], []
        for h in range(2):
            a = subs(high[h], 1)
            corner = lanes(subs(d_xpym[r, h], 1), -6)
            py_.append(jnp.where(sub > 0, a, jnp.where(in8 >= 2, lanes(a, 2), jnp.where(down[1], corner, high[h]))))
            pz_.append(jnp.where(in64 >= 8, lanes(high[h], 8),
                                 jnp.where(down[2], lanes(d_xpzm[r, h], -56), high[h])))
        new = q_step([qux[i] for i in range(6)], split(high)[1:],
                     [split(own_high)[1:], split(py_)[1:], split(pz_)[1:]])
        for i in range(6):
            qux[i] = new[i]
        above_x = [jnp.where(up[0], new[i], zero) for i in Q_OF[0]]

        inner, after, before = slice(1, NZ + 1), slice(2, NZ + 2), slice(0, NZ)
        here = bar[0, inner, 7, :]
        row = jnp.broadcast_to(d_xpym[r, 0, 7:8, :], (8, 128))
        col = jnp.sum(jnp.where(lane == 8 * sub + 6, row, 0.0), axis=1, keepdims=True)
        nx = jnp.where(lane < 127, lanes(here, -1), jnp.where(up[0], jnp.broadcast_to(col, (8, 128)), here))
        new = p_step([p[c, inner, 7, :] for c in range(3)], here,
                     [nx, bar[0, inner, 8, :], bar[0, after, 7, :]], [bar[1 + c, inner, 7, :] for c in range(3)])
        new[1] = jnp.where(down[1], new[1], zero)
        for c in range(3):
            p[c, inner, 7, :] = new[c]

        v = [bar[1 + c, inner, 8 + NY, :] for c in range(3)]
        bx = []
        for c in range(3):
            f = 1 + c
            row = jnp.broadcast_to(d_xmyp[r, f // 2, 0:1, :], (8, 128))
            source = lax.rem(8 * sub + (f % 2) * 64 + 127, 128)
            col = jnp.sum(jnp.where(lane == source, row, 0.0), axis=1, keepdims=True)
            bx.append(jnp.where(lane > 0, lanes(v[c], 1),
                                jnp.where(down[0], jnp.broadcast_to(col, (8, 128)), v[c])))
        new = q_step([q[i, before, NY, :] for i in range(6)], v,
                     [bx, [bar[1 + c, inner, 7 + NY, :] for c in range(3)],
                      [bar[1 + c, before, 8 + NY, :] for c in range(3)]])
        for i in range(6):
            q[i, before, NY, :] = jnp.where(up[1], new[i], zero) if i in Q_OF[1] else new[i]

        for t in EVERY:
            rows = slice(8 + 8 * t, 16 + 8 * t)
            here = bar[0, 0, rows, :]
            nx = jnp.where(lane < 127, lanes(here, -1),
                           jnp.where(up[0], lanes(d_xpzm[r, 0], 127 - 56 - 2 * t), here))
            new = p_step([p[c, 0, rows, :] for c in range(3)], here,
                         [nx, bar[0, 0, 9 + 8 * t : 17 + 8 * t, :], bar[0, 1, rows, :]],
                         [bar[1 + c, 0, rows, :] for c in range(3)])
            new[2] = jnp.where(down[2], new[2], zero)
            for c in range(3):
                p[c, 0, rows, :] = new[c]

            v = [bar[1 + c, NZ + 1, rows, :] for c in range(3)]
            bx = [jnp.where(lane > 0, lanes(v[c], 1),
                            jnp.where(down[0], lanes(d_xmzp[r, (1 + c) // 2], -((1 + c) % 2) * 64 - 2 * t + 1), v[c]))
                  for c in range(3)]
            new = q_step([q[i, NZ, 8 * t : 8 * t + 8, :] for i in range(6)], v,
                         [bx, [bar[1 + c, NZ + 1, 7 + 8 * t : 15 + 8 * t, :] for c in range(3)],
                          [bar[1 + c, NZ, rows, :] for c in range(3)]])
            for i in range(6):
                q[i, NZ, 8 * t : 8 * t + 8, :] = jnp.where(up[2], new[i], zero) if i in Q_OF[2] else new[i]
        return below_x, above_x

    def dual(r, tiles):
        bar = bars[r]
        high = xh_hi[r, 0]
        low = [xh_lo[r, h] for h in range(2)]
        for t in tiles:
            for z in range(NZ):
                rows = slice(8 + 8 * t, 16 + 8 * t)
                mine = slice(8 * t, 8 * t + 8)
                s = z * TILES + t
                here = bar[0, z + 1, rows, :]
                v = [bar[1 + c, z + 1, rows, :] for c in range(3)]
                nx = jnp.where(last, lanes(high, 127 - 2 * s), lanes(here, -1))
                new = p_step([p[c, z + 1, rows, :] for c in range(3)], here,
                             [nx, bar[0, z + 1, 9 + 8 * t : 17 + 8 * t, :], bar[0, z + 2, rows, :]], v)
                for c in range(3):
                    p[c, z + 1, rows, :] = new[c]
                bx = [jnp.where(first, lanes(low[(1 + c) // 2], 1 - ((1 + c) % 2) * 64 - 2 * s), lanes(v[c], 1))
                      for c in range(3)]
                new = q_step([q[i, z, mine, :] for i in range(6)], v,
                             [bx, [bar[1 + c, z + 1, 7 + 8 * t : 15 + 8 * t, :] for c in range(3)],
                              [bar[1 + c, z, rows, :] for c in range(3)]])
                for i in range(6):
                    q[i, z, mine, :] = new[i]

    def primal(r, tiles, acc, below_x, above_x):
        for t in tiles:
            for z in range(NZ):
                rows = slice(8 + 8 * t, 16 + 8 * t)
                mine = slice(8 * t, 8 * t + 8)
                if r == 0:
                    old = [bar0[f, z + 1, rows, :] for f in range(4)]
                else:
                    old = [uv[f, z, mine, :] for f in range(4)]
                new, values = primal_tile(z, t, masks, p, q, old, (fa[z, mine, :], wb[z, mine, :]), below_x, above_x)
                for f in range(4):
                    uv[f, z, mine, :] = new[f]
                    bars[r + 1][f, z + 1, rows, :] = values[f]
                pack_into(acc, z, t, values, edge, 0)

    for r in range(ITERS):
        receive(r, NEAR0 if r == 0 else NEAR)
        clamp_near(r)
        if r == 0:
            for c in range(3):
                plx[c] = lanes(plxk[c // 2], (c % 2) * 64)
            for i in range(6):
                qux[i] = lanes(quxk[i // 2], (i % 2) * 64)
        dual(r, INNER)
        receive(r, FAR0 if r == 0 else FAR)
        clamp_far(r)
        below_x, above_x = layers(r)
        dual(r, OUTER)
        if r < ITERS - 1:
            acc = [zero, zero]
            primal(r, OUTER, acc, below_x, above_x)
            for h in range(2):
                xey[r + 1, h] = acc[h]
            send(r + 1, FAR)
            primal(r, INNER, acc, below_x, above_x)
            for h in range(2):
                xe[r + 1, h] = acc[h]
            send(r + 1, NEAR)
    cols[0] = below_x
    for j in range(3):
        cols[1 + j] = above_x[j]
    for r in range(ITERS):
        for m in (FAR0 + NEAR0 if r == 0 else FAR + NEAR):
            @pl.when(exists(MOVES[m]))
            def _():
                message(m, r).wait_send()


def final_kernel(sizes, uv, p, q, fa, wb, cols, u_out, v_out, p_out, q_out, new_uv, out_sem):
    _, up, down = place(sizes)
    masks = edge_masks(up, down)
    stores = [
        pltpu.make_async_copy(p.at[:, 1 : NZ + 1, 8 : 8 + NY, :], p_out, out_sem.at[0]),
        pltpu.make_async_copy(q.at[:, 0:NZ, 0:NY, :], q_out, out_sem.at[1]),
    ]
    for c in stores:
        c.start()
    below_x = cols[0]
    above_x = [cols[1 + j] for j in range(3)]
    for z in range(NZ):
        for t in EVERY:
            mine = slice(8 * t, 8 * t + 8)
            new, _ = primal_tile(z, t, masks, p, q, [uv[f, z, mine, :] for f in range(4)],
                                 (fa[z, mine, :], wb[z, mine, :]), below_x, above_x)
            for f in range(4):
                new_uv[f, z, mine, :] = new[f]
        if z % 4 == 3:
            part = slice(z - 3, z + 1)
            more = [
                pltpu.make_async_copy(new_uv.at[0, part], u_out.at[part], out_sem.at[2 + z // 4]),
                pltpu.make_async_copy(new_uv.at[1:4, part], v_out.at[:, part], out_sem.at[4 + z // 4]),
            ]
            for c in more:
                c.start()
            stores += more
    for c in stores:
        c.wait()


def per_device(sizes, *arrays):
    hbm = pl.BlockSpec(memory_space=pltpu.HBM)
    here = pl.BlockSpec(memory_space=pltpu.VMEM)
    tile = (8, 128)

    def vmem(*shape):
        return pltpu.VMEM(shape, F32)

    state = pl.pallas_call(
        functools.partial(exchange_kernel, sizes),
        out_shape=(
            vmem(4, NZ, NY, NX),
            vmem(3, NZ + 1, PROWS, NX),
            vmem(6, NZ + 1, PROWS, NX),
            vmem(NZ, NY, NX),
            vmem(NZ, NY, NX),
            vmem(4, *tile),
        ),
        in_specs=[hbm] * 6,
        out_specs=(here,) * 6,
        scratch_shapes=[
            vmem(4, NZ + 2, ROWS, NX), vmem(4, NZ + 2, ROWS, NX), vmem(4, NZ + 2, ROWS, NX),
            vmem(ITERS, 2, *tile), vmem(ITERS, 2, *tile),
            vmem(ITERS, 2, *tile), vmem(ITERS, 2, *tile),
            vmem(ITERS, 2, *tile), vmem(ITERS, 2, *tile), vmem(ITERS, 2, *tile), vmem(ITERS, 2, *tile),
            vmem(2, *tile), vmem(3, *tile), vmem(2, *tile), vmem(3, *tile),
            vmem(3, *tile), vmem(6, *tile),
            pltpu.SemaphoreType.DMA((6,)),
            pltpu.SemaphoreType.DMA((ITERS, 18)),
            pltpu.SemaphoreType.DMA((ITERS, 18)),
        ],
        compiler_params=pltpu.CompilerParams(
            collective_id=0, has_side_effects=True, vmem_limit_bytes=24 << 20
        ),
        name="tgv_rounds",
    )(*[pltpu.with_memory_space_constraint(a, pltpu.HBM) for a in arrays])
    return pl.pallas_call(
        functools.partial(final_kernel, sizes),
        out_shape=tuple(jax.ShapeDtypeStruct(s, F32) for s in
                        ((NZ, NY, NX), (3, NZ, NY, NX), (3, NZ, NY, NX), (6, NZ, NY, NX))),
        in_specs=[here] * 6,
        out_specs=(hbm,) * 4,
        scratch_shapes=[vmem(4, NZ, NY, NX), pltpu.SemaphoreType.DMA((6,))],
        compiler_params=pltpu.CompilerParams(vmem_limit_bytes=24 << 20),
        name="tgv_last",
    )(*state)


def solution(mesh):
    sizes = tuple(mesh.shape[n] for n in NAMES)
    scalar = P("gz", "gy", "gx")
    stack = P(None, "gz", "gy", "gx")
    return jax.shard_map(
        functools.partial(per_device, sizes), mesh=mesh,
        in_specs=(scalar, scalar, scalar, stack, stack, stack),
        out_specs=(scalar, stack, stack, stack), check_vma=False,
    )
```

```python
import functools

import jax
import jax.numpy as jnp
from jax import lax
from jax.experimental import pallas as pl
from jax.experimental.pallas import tpu as pltpu
from jax.sharding import PartitionSpec as P

ITERS = 3
SIGMA = 0.2
TAU = 0.2
ALPHA1 = 0.5
ALPHA0 = 1.0
NZ, NY, NX = 8, 32, 128
TILES = NY // 8
ROWS = NY + 16
PROWS = NY + 8
Q_OF = ((0, 3, 4), (3, 1, 5), (4, 5, 2))
F32 = jnp.float32
NAMES = ("gx", "gy", "gz")

(ZUP, ZDN, YUP, YDN, XUP, XDN, XUP_YDN, XDN_YUP, XUP_ZDN, XDN_ZUP, YUP_ZDN, YDN_ZUP,
 PZ, QZ, PY, QY, PX_, QX_) = range(18)
MOVES = {
    ZUP: (0, 0, 1), ZDN: (0, 0, -1), YUP: (0, 1, 0), YDN: (0, -1, 0), XUP: (1, 0, 0), XDN: (-1, 0, 0),
    XUP_YDN: (1, -1, 0), XDN_YUP: (-1, 1, 0), XUP_ZDN: (1, 0, -1), XDN_ZUP: (-1, 0, 1),
    YUP_ZDN: (0, 1, -1), YDN_ZUP: (0, -1, 1),
    PZ: (0, 0, 1), QZ: (0, 0, -1), PY: (0, 1, 0), QY: (0, -1, 0), PX_: (1, 0, 0), QX_: (-1, 0, 0),
}
N_BAR = 12
FAR = (XUP_YDN, XDN_YUP, YUP, YDN, YUP_ZDN, YDN_ZUP)
NEAR = (ZDN, ZUP, XUP, XDN, XUP_ZDN, XDN_ZUP)
FAR0 = FAR + (QY, PY)
NEAR0 = NEAR + (QZ, PZ, PX_, QX_)
INNER = tuple(range(1, TILES - 1))
OUTER = (0, TILES - 1)
EVERY = tuple(range(TILES))


def p_step(p, here, following, v):
    t = [p[a] + SIGMA * ((following[a] - here) - v[a]) for a in range(3)]
    size = t[0] * t[0] + t[1] * t[1] + t[2] * t[2]
    scale = jnp.minimum(1.0, ALPHA1 * lax.rsqrt(size))
    return [scale * t[a] for a in range(3)]


def q_step(q, v, before):
    d = [[v[a] - before[b][a] for a in range(3)] for b in range(3)]
    s = [q[a] + SIGMA * d[a][a] for a in range(3)]
    s.append(q[3] + (0.5 * SIGMA) * (d[1][0] + d[0][1]))
    s.append(q[4] + (0.5 * SIGMA) * (d[2][0] + d[0][2]))
    s.append(q[5] + (0.5 * SIGMA) * (d[2][1] + d[1][2]))
    size = (s[0] * s[0] + s[1] * s[1] + s[2] * s[2]) + 2.0 * (s[3] * s[3] + s[4] * s[4] + s[5] * s[5])
    scale = jnp.minimum(1.0, ALPHA0 * lax.rsqrt(size))
    return [scale * s[i] for i in range(6)]


def lanes(x, by):
    return x if by % 128 == 0 else pltpu.roll(x, by % 128, 1)


def subs(x, by):
    return pltpu.roll(x, by % 8, 0)


def tile_iota(axis):
    return lax.broadcasted_iota(jnp.int32, (8, 128), axis)


def place(sizes):
    at = [lax.axis_index(n) for n in NAMES]
    return at, [at[i] < sizes[i] - 1 for i in range(3)], [at[i] > 0 for i in range(3)]


def primal_tile(z, t, masks, p, q, old, weight, below_x, above_x):
    first, last = masks[6], masks[7]
    rows = slice(8 + 8 * t, 16 + 8 * t)
    mine = slice(8 * t, 8 * t + 8)
    s = z * TILES + t
    pv = [p[c, z + 1, rows, :] for c in range(3)]
    div = masks[0] * pv[0] - jnp.where(first, lanes(below_x, -2 * s), lanes(pv[0], 1))
    div = div + ((masks[2] * pv[1] if t == TILES - 1 else pv[1]) - p[1, z + 1, 7 + 8 * t : 15 + 8 * t, :])
    div = div + ((masks[4] * pv[2] if z == NZ - 1 else pv[2]) - p[2, z, rows, :])
    fw, inverse = weight
    new = [(old[0] + TAU * div + fw) * inverse]
    bars = [2.0 * new[0] - old[0]]
    qv = [q[i, z, mine, :] for i in range(6)]
    qn = [jnp.where(last, lanes(above_x[j], 127 - 2 * s), lanes(qv[i], -1)) for j, i in enumerate(Q_OF[0])]
    for a in range(3):
        ix, iy, iz = Q_OF[a]
        total = pv[a] + (qn[a] - masks[1] * qv[ix])
        total = total + (q[iy, z, 1 + 8 * t : 9 + 8 * t, :] - (masks[3] * qv[iy] if t == 0 else qv[iy]))
        total = total + (q[iz, z + 1, mine, :] - (masks[5] * qv[iz] if z == 0 else qv[iz]))
        step = TAU * total
        new.append(old[1 + a] + step)
        bars.append(new[1 + a] + step)
    return new, bars


def edge_masks(up, down):
    lane, sub = tile_iota(1), tile_iota(0)
    first, last = lane == 0, lane == 127

    def at(where, inside):
        return jnp.where(jnp.logical_and(where, jnp.logical_not(inside)), 0.0, 1.0).astype(F32)

    return (at(last, up[0]), at(first, down[0]), at(sub == 7, up[1]), at(sub == 0, down[1]),
            jnp.where(up[2], 1.0, 0.0).astype(F32), jnp.where(down[2], 1.0, 0.0).astype(F32), first, last)


def exchange_kernel(sizes, f_in, w_in, u_in, v_in, p_in, q_in,
                    uv, p, q, fa, wb, cols,
                    bar0, bar1, bar2, xe, kept, xh_lo, xh_hi, d_xmyp, d_xpym, d_xmzp, d_xpzm,
                    pxk, qxk, plxk, quxk, plx, qux,
                    in_sem, send_sem, recv_sem):
    at, up, down = place(sizes)
    bars = (bar0, bar1, bar2)

    def exists(move):
        flag = None
        for i in range(3):
            if move[i]:
                one = up[i] if move[i] > 0 else down[i]
                flag = one if flag is None else jnp.logical_and(flag, one)
        return flag

    def device(move):
        return {NAMES[i]: at[i] + move[i] for i in range(3) if move[i]}

    def opposite(move):
        return tuple(-m for m in move)

    loads = [
        pltpu.make_async_copy(u_in, bar0.at[0, 1 : NZ + 1, 8 : 8 + NY, :], in_sem.at[0]),
        pltpu.make_async_copy(v_in, bar0.at[1:4, 1 : NZ + 1, 8 : 8 + NY, :], in_sem.at[1]),
        pltpu.make_async_copy(p_in, p.at[:, 1 : NZ + 1, 8 : 8 + NY, :], in_sem.at[2]),
        pltpu.make_async_copy(q_in, q.at[:, 0:NZ, 0:NY, :], in_sem.at[3]),
        pltpu.make_async_copy(f_in, fa, in_sem.at[4]),
        pltpu.make_async_copy(w_in, wb, in_sem.at[5]),
    ]
    barrier = pltpu.get_barrier_semaphore()
    arrivals = jnp.int32(0)
    for m in FAR + NEAR:
        move = MOVES[m]
        arrivals = arrivals + exists(move).astype(jnp.int32)

        @pl.when(exists(move))
        def _():
            pl.semaphore_signal(
                barrier, inc=1, device_id=device(move), device_id_type=pl.DeviceIdType.MESH
            )

    for c in loads:
        c.start()

    def ends(m, r):
        bar = bars[r]
        inner = slice(1, NZ + 1)
        if m == ZUP:
            return bar.at[:, NZ, 8 : 8 + NY, :], bar.at[:, 0, 8 : 8 + NY, :]
        if m == ZDN:
            return bar.at[:, 1, 8 : 8 + NY, :], bar.at[:, NZ + 1, 8 : 8 + NY, :]
        if m == YUP:
            return bar.at[:, 1 : NZ + 1, 7 + NY, :], bar.at[:, 1 : NZ + 1, 7, :]
        if m == YDN:
            return bar.at[:, 1 : NZ + 1, 8, :], bar.at[:, 1 : NZ + 1, 8 + NY, :]
        if m == YUP_ZDN:
            return bar.at[:, 1, 7 + NY, :], bar.at[:, NZ + 1, 7, :]
        if m == YDN_ZUP:
            return bar.at[:, NZ, 8, :], bar.at[:, 0, 8 + NY, :]
        if m == PZ:
            return p_in.at[:, NZ - 1, :, :], p.at[:, 0, 8 : 8 + NY, :]
        if m == QZ:
            return q_in.at[:, 0, :, :], q.at[:, NZ, 0:NY, :]
        if m == PY:
            return p_in.at[:, :, NY - 1, :], p.at[:, 1 : NZ + 1, 7, :]
        if m == QY:
            return q_in.at[:, :, 0, :], q.at[:, 0:NZ, NY, :]
        if m == XUP_YDN:
            return xe.at[r, :, 0, :], d_xmyp.at[r, :, 0, :]
        if m == XDN_YUP:
            return xe.at[r, :, 7, :], d_xpym.at[r, :, 7, :]
        if m == PX_:
            return pxk, plxk
        if m == QX_:
            return qxk, quxk
        src, dst = {
            XUP: (xe, xh_lo), XDN: (xe, xh_hi),
            XUP_ZDN: (xe, d_xmzp), XDN_ZUP: (xe, d_xpzm),
        }[m]
        return src.at[r], dst.at[r]

    def message(m, r):
        src, dst = ends(m, r)
        return pltpu.make_async_remote_copy(
            src_ref=src, dst_ref=dst, send_sem=send_sem.at[r, m], recv_sem=recv_sem.at[r, m],
            device_id=device(MOVES[m]), device_id_type=pl.DeviceIdType.MESH,
        )

    def send(r, which):
        for m in which:
            @pl.when(exists(MOVES[m]))
            def _():
                message(m, r).start()

    def receive(r, which):
        for m in which:
            @pl.when(exists(opposite(MOVES[m])))
            def _():
                message(m, r).wait_recv()

    lane, sub = tile_iota(1), tile_iota(0)
    first, last = lane == 0, lane == 127
    edge = jnp.logical_or(first, last)
    zero = jnp.zeros((8, 128), F32)
    masks = edge_masks(up, down)

    def pack_into(acc, z, t, values, mask, by):
        for f, x in enumerate(values):
            acc[f // 2] = acc[f // 2] + lanes(jnp.where(mask, x, 0.0), (f % 2) * 64 + 2 * (z * TILES + t) + by)

    loads[0].wait()
    loads[1].wait()
    acc = [zero, zero]
    for t in OUTER + INNER:
        for z in range(NZ):
            pack_into(acc, z, t, [bar0[f, z + 1, 8 + 8 * t : 16 + 8 * t, :] for f in range(4)], edge, 0)
    for h in range(2):
        xe[0, h] = acc[h]
    loads[2].wait()
    loads[3].wait()
    accp, accq = [zero, zero], [zero, zero, zero]
    for t in EVERY:
        for z in range(NZ):
            pack_into(accp, z, t, [p[a, z + 1, 8 + 8 * t : 16 + 8 * t, :] for a in range(3)], last, 1)
            pack_into(accq, z, t, [q[i, z, 8 * t : 8 * t + 8, :] for i in range(6)], first, 0)
    for h in range(2):
        pxk[h] = accp[h]
    for h in range(3):
        qxk[h] = accq[h]

    pl.semaphore_wait(barrier, arrivals)
    send(0, FAR0)
    send(0, NEAR0)

    loads[4].wait()
    loads[5].wait()
    for z in range(NZ):
        for t in EVERY:
            rows = slice(8 * t, 8 * t + 8)
            tw = TAU * wb[z, rows, :]
            fa[z, rows, :] = tw * fa[z, rows, :]
            wb[z, rows, :] = 1.0 / (1.0 + tw)

    def split(x):
        return [x[0], lanes(x[0], 64), x[1], lanes(x[1], 64)]

    def clamp_near(r):
        bar = bars[r]

        @pl.when(jnp.logical_not(up[0]))
        def _():
            for h in range(2):
                xh_hi[r, h] = lanes(xe[r, h], 1)

        @pl.when(jnp.logical_not(down[0]))
        def _():
            for h in range(2):
                xh_lo[r, h] = lanes(xe[r, h], -1)

        @pl.when(jnp.logical_not(up[2]))
        def _():
            bar[:, NZ + 1, 8 : 8 + NY, :] = bar[:, NZ, 8 : 8 + NY, :]

        @pl.when(jnp.logical_not(down[2]))
        def _():
            bar[:, 0, 8 : 8 + NY, :] = bar[:, 1, 8 : 8 + NY, :]

    def clamp_far(r):
        bar = bars[r]

        @pl.when(jnp.logical_not(up[2]))
        def _():
            for f in range(4):
                bar[f, NZ + 1, 7:8, :] = bar[f, NZ, 7:8, :]

        @pl.when(jnp.logical_not(down[2]))
        def _():
            for f in range(4):
                bar[f, 0, 8 + NY : 9 + NY, :] = bar[f, 1, 8 + NY : 9 + NY, :]

        @pl.when(jnp.logical_not(up[1]))
        def _():
            for f in range(4):
                bar[f, 0, 8 + NY : 9 + NY, :] = bar[f, 0, 7 + NY : 8 + NY, :]
                bar[f, 1 : NZ + 1, 8 + NY, :] = bar[f, 1 : NZ + 1, 7 + NY, :]

        @pl.when(jnp.logical_not(down[1]))
        def _():
            for f in range(4):
                bar[f, NZ + 1, 7:8, :] = bar[f, NZ + 1, 8:9, :]
                bar[f, 1 : NZ + 1, 7, :] = bar[f, 1 : NZ + 1, 8, :]

    in64 = lax.rem(lane, 64)
    in8 = lax.rem(lane, 8)

    def x_layers(r, corners):
        own = [xe[r, h] for h in range(2)]
        own_high = [lanes(x, 1) for x in own]
        low = [lanes(xh_lo[r, h], 1) for h in range(2)]
        here = low[0]
        a = subs(here, -1)
        corner = jnp.where(up[1], lanes(subs(d_xmyp[r, 0], -1), 7), here) if corners else here
        ny = jnp.where(sub < 7, a, jnp.where(in8 < 6, lanes(a, -2), corner))
        nz = jnp.where(in64 < 56, lanes(here, -8), jnp.where(up[2], lanes(d_xmzp[r, 0], 57), here))
        new = p_step([plx[c] for c in range(3)], here, [own[0], ny, nz], split(low)[1:])
        if corners:
            for c in range(3):
                plx[c] = new[c]
        below_x = jnp.where(down[0], new[0], zero)

        high = [xh_hi[r, h] for h in range(2)]
        py_, pz_ = [], []
        for h in range(2):
            a = subs(high[h], 1)
            corner = jnp.where(down[1], lanes(subs(d_xpym[r, h], 1), -6), high[h]) if corners else high[h]
            py_.append(jnp.where(sub > 0, a, jnp.where(in8 >= 2, lanes(a, 2), corner)))
            pz_.append(jnp.where(in64 >= 8, lanes(high[h], 8),
                                 jnp.where(down[2], lanes(d_xpzm[r, h], -56), high[h])))
        new = q_step([qux[i] for i in range(6)], split(high)[1:],
                     [split(own_high)[1:], split(py_)[1:], split(pz_)[1:]])
        if corners:
            for i in range(6):
                qux[i] = new[i]
        return below_x, [jnp.where(up[0], new[i], zero) for i in Q_OF[0]]

    def high_column(source, f):
        row = jnp.broadcast_to(source[f // 2, 0:1, :], (8, 128))
        picked = jnp.where(lane == lax.rem(8 * sub + (f % 2) * 64 + 127, 128), row, 0.0)
        return jnp.broadcast_to(jnp.sum(picked, axis=1, keepdims=True), (8, 128))

    def low_column(source):
        row = jnp.broadcast_to(source[0, 7:8, :], (8, 128))
        return jnp.broadcast_to(jnp.sum(jnp.where(lane == 8 * sub + 6, row, 0.0), axis=1, keepdims=True), (8, 128))

    inner, after, before = slice(1, NZ + 1), slice(2, NZ + 2), slice(0, NZ)

    def keep_rows(r):
        for c in range(3):
            kept[c] = p[c, inner, 7 + NY, :]
            kept[10 + c] = high_column(xh_lo.at[r], 1 + c)
        for i in range(6):
            kept[3 + i] = q[i, before, 0, :]
        kept[9] = low_column(xh_hi.at[r])

    def redo_rows(r):
        bar = bars[r]
        here = bar[0, inner, 7 + NY, :]
        nx = jnp.where(last, kept[9], lanes(here, -1))
        new = p_step([kept[c] for c in range(3)], here, [nx, bar[0, inner, 8 + NY, :], bar[0, after, 7 + NY, :]],
                     [bar[1 + c, inner, 7 + NY, :] for c in range(3)])
        for c in range(3):
            p[c, inner, 7 + NY, :] = new[c]
        v = [bar[1 + c, inner, 8, :] for c in range(3)]
        bx = [jnp.where(first, kept[10 + c], lanes(v[c], 1)) for c in range(3)]
        new = q_step([kept[3 + i] for i in range(6)], v,
                     [bx, [bar[1 + c, inner, 7, :] for c in range(3)], [bar[1 + c, before, 8, :] for c in range(3)]])
        for i in range(6):
            q[i, before, 0, :] = new[i]

    def y_layers(r):
        bar = bars[r]
        here = bar[0, inner, 7, :]
        nx = jnp.where(lane < 127, lanes(here, -1), jnp.where(up[0], low_column(d_xpym.at[r]), here))
        new = p_step([p[c, inner, 7, :] for c in range(3)], here,
                     [nx, bar[0, inner, 8, :], bar[0, after, 7, :]], [bar[1 + c, inner, 7, :] for c in range(3)])
        new[1] = jnp.where(down[1], new[1], zero)
        for c in range(3):
            p[c, inner, 7, :] = new[c]

        v = [bar[1 + c, inner, 8 + NY, :] for c in range(3)]
        bx = [jnp.where(lane > 0, lanes(v[c], 1), jnp.where(down[0], high_column(d_xmyp.at[r], 1 + c), v[c]))
              for c in range(3)]
        new = q_step([q[i, before, NY, :] for i in range(6)], v,
                     [bx, [bar[1 + c, inner, 7 + NY, :] for c in range(3)],
                      [bar[1 + c, before, 8 + NY, :] for c in range(3)]])
        for i in range(6):
            q[i, before, NY, :] = jnp.where(up[1], new[i], zero) if i in Q_OF[1] else new[i]

    def z_layers(r, tiles):
        bar = bars[r]
        for t in tiles:
            rows = slice(8 + 8 * t, 16 + 8 * t)
            here = bar[0, 0, rows, :]
            nx = jnp.where(lane < 127, lanes(here, -1),
                           jnp.where(up[0], lanes(d_xpzm[r, 0], 127 - 56 - 2 * t), here))
            new = p_step([p[c, 0, rows, :] for c in range(3)], here,
                         [nx, bar[0, 0, 9 + 8 * t : 17 + 8 * t, :], bar[0, 1, rows, :]],
                         [bar[1 + c, 0, rows, :] for c in range(3)])
            new[2] = jnp.where(down[2], new[2], zero)
            for c in range(3):
                p[c, 0, rows, :] = new[c]

            v = [bar[1 + c, NZ + 1, rows, :] for c in range(3)]
            bx = [jnp.where(lane > 0, lanes(v[c], 1),
                            jnp.where(down[0], lanes(d_xmzp[r, (1 + c) // 2], -((1 + c) % 2) * 64 - 2 * t + 1), v[c]))
                  for c in range(3)]
            new = q_step([q[i, NZ, 8 * t : 8 * t + 8, :] for i in range(6)], v,
                         [bx, [bar[1 + c, NZ + 1, 7 + 8 * t : 15 + 8 * t, :] for c in range(3)],
                          [bar[1 + c, NZ, rows, :] for c in range(3)]])
            for i in range(6):
                q[i, NZ, 8 * t : 8 * t + 8, :] = jnp.where(up[2], new[i], zero) if i in Q_OF[2] else new[i]

    def dual(r, tiles):
        bar = bars[r]
        high = xh_hi[r, 0]
        low = [xh_lo[r, h] for h in range(2)]
        for t in tiles:
            for z in range(NZ):
                rows = slice(8 + 8 * t, 16 + 8 * t)
                mine = slice(8 * t, 8 * t + 8)
                s = z * TILES + t
                here = bar[0, z + 1, rows, :]
                v = [bar[1 + c, z + 1, rows, :] for c in range(3)]
                nx = jnp.where(last, lanes(high, 127 - 2 * s), lanes(here, -1))
                ny = subs(here, -1) if t == TILES - 1 else bar[0, z + 1, 9 + 8 * t : 17 + 8 * t, :]
                by = [subs(v[c], 1) if t == 0 else bar[1 + c, z + 1, 7 + 8 * t : 15 + 8 * t, :] for c in range(3)]
                new = p_step([p[c, z + 1, rows, :] for c in range(3)], here,
                             [nx, ny, bar[0, z + 2, rows, :]], v)
                for c in range(3):
                    p[c, z + 1, rows, :] = new[c]
                bx = [jnp.where(first, lanes(low[(1 + c) // 2], 1 - ((1 + c) % 2) * 64 - 2 * s), lanes(v[c], 1))
                      for c in range(3)]
                new = q_step([q[i, z, mine, :] for i in range(6)], v,
                             [bx, by, [bar[1 + c, z, rows, :] for c in range(3)]])
                for i in range(6):
                    q[i, z, mine, :] = new[i]

    def primal(r, tiles, acc, below_x, above_x):
        for t in tiles:
            for z in range(NZ):
                rows = slice(8 + 8 * t, 16 + 8 * t)
                mine = slice(8 * t, 8 * t + 8)
                if r == 0:
                    old = [bar0[f, z + 1, rows, :] for f in range(4)]
                else:
                    old = [uv[f, z, mine, :] for f in range(4)]
                new, values = primal_tile(z, t, masks, p, q, old, (fa[z, mine, :], wb[z, mine, :]), below_x, above_x)
                for f in range(4):
                    uv[f, z, mine, :] = new[f]
                    if r < ITERS - 1:
                        bars[r + 1][f, z + 1, rows, :] = values[f]
                if r < ITERS - 1:
                    pack_into(acc, z, t, values, edge, 0)

    for r in range(ITERS):
        receive(r, NEAR0 if r == 0 else NEAR)
        clamp_near(r)
        if r == 0:
            for c in range(3):
                plx[c] = lanes(plxk[c // 2], (c % 2) * 64)
            for i in range(6):
                qux[i] = lanes(quxk[i // 2], (i % 2) * 64)
        keep_rows(r)
        dual(r, EVERY)
        z_layers(r, INNER)
        acc = [zero, zero]
        primal(r, INNER, acc, *x_layers(r, False))
        receive(r, FAR0 if r == 0 else FAR)
        clamp_far(r)
        below_x, above_x = x_layers(r, True)
        y_layers(r)
        z_layers(r, OUTER)
        redo_rows(r)
        if r < ITERS - 1:
            primal(r, OUTER, acc, below_x, above_x)
            for h in range(2):
                xe[r + 1, h] = acc[h]
            send(r + 1, FAR)
            send(r + 1, NEAR)
    cols[0] = below_x
    for j in range(3):
        cols[1 + j] = above_x[j]
    for r in range(ITERS):
        for m in (FAR0 + NEAR0 if r == 0 else FAR + NEAR):
            @pl.when(exists(MOVES[m]))
            def _():
                message(m, r).wait_send()


def final_kernel(sizes, uv, p, q, fa, wb, cols, u_out, v_out, p_out, q_out, new_uv, out_sem):
    _, up, down = place(sizes)
    masks = edge_masks(up, down)
    stores = [
        pltpu.make_async_copy(p.at[:, 1 : NZ + 1, 8 : 8 + NY, :], p_out, out_sem.at[0]),
        pltpu.make_async_copy(q.at[:, 0:NZ, 0:NY, :], q_out, out_sem.at[1]),
    ]
    for c in stores:
        c.start()
    middle = slice(8, NY - 8)
    more = [
        pltpu.make_async_copy(uv.at[0, :, middle, :], u_out.at[:, middle, :], out_sem.at[2]),
        pltpu.make_async_copy(uv.at[1:4, :, middle, :], v_out.at[:, :, middle, :], out_sem.at[3]),
    ]
    for c in more:
        c.start()
    stores += more
    below_x = cols[0]
    above_x = [cols[1 + j] for j in range(3)]
    for k, t in enumerate(OUTER):
        mine = slice(8 * t, 8 * t + 8)
        for z in range(NZ):
            new, _ = primal_tile(z, t, masks, p, q, [uv[f, z, mine, :] for f in range(4)],
                                 (fa[z, mine, :], wb[z, mine, :]), below_x, above_x)
            for f in range(4):
                new_uv[k, f, z] = new[f]
        more = [
            pltpu.make_async_copy(new_uv.at[k, 0], u_out.at[:, mine, :], out_sem.at[4 + k]),
            pltpu.make_async_copy(new_uv.at[k, 1:4], v_out.at[:, :, mine, :], out_sem.at[6 + k]),
        ]
        for c in more:
            c.start()
        stores += more
    for c in stores:
        c.wait()


def per_device(sizes, *arrays):
    hbm = pl.BlockSpec(memory_space=pltpu.HBM)
    here = pl.BlockSpec(memory_space=pltpu.VMEM)
    tile = (8, 128)

    def vmem(*shape):
        return pltpu.VMEM(shape, F32)

    state = pl.pallas_call(
        functools.partial(exchange_kernel, sizes),
        out_shape=(
            vmem(4, NZ, NY, NX),
            vmem(3, NZ + 1, PROWS, NX),
            vmem(6, NZ + 1, PROWS, NX),
            vmem(NZ, NY, NX),
            vmem(NZ, NY, NX),
            vmem(4, *tile),
        ),
        in_specs=[hbm] * 6,
        out_specs=(here,) * 6,
        scratch_shapes=[
            vmem(4, NZ + 2, ROWS, NX), vmem(4, NZ + 2, ROWS, NX), vmem(4, NZ + 2, ROWS, NX),
            vmem(ITERS, 2, *tile), vmem(13, *tile),
            vmem(ITERS, 2, *tile), vmem(ITERS, 2, *tile),
            vmem(ITERS, 2, *tile), vmem(ITERS, 2, *tile), vmem(ITERS, 2, *tile), vmem(ITERS, 2, *tile),
            vmem(2, *tile), vmem(3, *tile), vmem(2, *tile), vmem(3, *tile),
            vmem(3, *tile), vmem(6, *tile),
            pltpu.SemaphoreType.DMA((6,)),
            pltpu.SemaphoreType.DMA((ITERS, 18)),
            pltpu.SemaphoreType.DMA((ITERS, 18)),
        ],
        compiler_params=pltpu.CompilerParams(
            collective_id=0, has_side_effects=True, vmem_limit_bytes=24 << 20
        ),
        name="tgv_rounds",
    )(*[pltpu.with_memory_space_constraint(a, pltpu.HBM) for a in arrays])
    return pl.pallas_call(
        functools.partial(final_kernel, sizes),
        out_shape=tuple(jax.ShapeDtypeStruct(s, F32) for s in
                        ((NZ, NY, NX), (3, NZ, NY, NX), (3, NZ, NY, NX), (6, NZ, NY, NX))),
        in_specs=[here] * 6,
        out_specs=(hbm,) * 4,
        scratch_shapes=[vmem(2, 4, NZ, *tile), pltpu.SemaphoreType.DMA((8,))],
        compiler_params=pltpu.CompilerParams(vmem_limit_bytes=24 << 20),
        name="tgv_last",
    )(*state)


def solution(mesh):
    sizes = tuple(mesh.shape[n] for n in NAMES)
    scalar = P("gz", "gy", "gx")
    stack = P(None, "gz", "gy", "gx")
    return jax.shard_map(
        functools.partial(per_device, sizes), mesh=mesh,
        in_specs=(scalar, scalar, scalar, stack, stack, stack),
        out_specs=(scalar, stack, stack, stack), check_vma=False,
    )
```

```python
import functools

import jax
import jax.numpy as jnp
from jax import lax
from jax.experimental import pallas as pl
from jax.experimental.pallas import tpu as pltpu
from jax.sharding import PartitionSpec as P

ITERS = 3
SIGMA = 0.2
TAU = 0.2
ALPHA1 = 0.5
ALPHA0 = 1.0
NZ, NY, NX = 8, 32, 128
TILES = NY // 8
ROWS = NY + 16
PROWS = NY + 8
Q_OF = ((0, 3, 4), (3, 1, 5), (4, 5, 2))
F32 = jnp.float32
NAMES = ("gx", "gy", "gz")

(ZUP, ZDN, YUP, YDN, XUP, XDN, XUP_YDN, XDN_YUP, XUP_ZDN, XDN_ZUP, YUP_ZDN, YDN_ZUP,
 PZ, QZ, PY, QY, PX_, QX_) = range(18)
MOVES = {
    ZUP: (0, 0, 1), ZDN: (0, 0, -1), YUP: (0, 1, 0), YDN: (0, -1, 0), XUP: (1, 0, 0), XDN: (-1, 0, 0),
    XUP_YDN: (1, -1, 0), XDN_YUP: (-1, 1, 0), XUP_ZDN: (1, 0, -1), XDN_ZUP: (-1, 0, 1),
    YUP_ZDN: (0, 1, -1), YDN_ZUP: (0, -1, 1),
    PZ: (0, 0, 1), QZ: (0, 0, -1), PY: (0, 1, 0), QY: (0, -1, 0), PX_: (1, 0, 0), QX_: (-1, 0, 0),
}
N_BAR = 12
LOWER = (XDN_YUP, YUP, YUP_ZDN)
UPPER = (XUP_YDN, YDN, YDN_ZUP)
ALONG_X = (XUP, XDN)
ALONG_Z = (XUP_ZDN, XDN_ZUP, ZDN, ZUP)
LOWER0, UPPER0 = LOWER + (PY,), UPPER + (QY,)
ALONG_X0, ALONG_Z0 = ALONG_X + (PX_, QX_), ALONG_Z + (QZ, PZ)
ALL = LOWER + UPPER + ALONG_X + ALONG_Z
ALL0 = LOWER0 + UPPER0 + ALONG_X0 + ALONG_Z0
INNER = tuple(range(1, TILES - 1))
OUTER = (0, TILES - 1)
EVERY = tuple(range(TILES))


def p_step(p, here, following, v):
    t = [p[a] + SIGMA * ((following[a] - here) - v[a]) for a in range(3)]
    size = t[0] * t[0] + t[1] * t[1] + t[2] * t[2]
    scale = jnp.minimum(1.0, ALPHA1 * lax.rsqrt(size))
    return [scale * t[a] for a in range(3)]


def q_step(q, v, before):
    d = [[v[a] - before[b][a] for a in range(3)] for b in range(3)]
    s = [q[a] + SIGMA * d[a][a] for a in range(3)]
    s.append(q[3] + (0.5 * SIGMA) * (d[1][0] + d[0][1]))
    s.append(q[4] + (0.5 * SIGMA) * (d[2][0] + d[0][2]))
    s.append(q[5] + (0.5 * SIGMA) * (d[2][1] + d[1][2]))
    size = (s[0] * s[0] + s[1] * s[1] + s[2] * s[2]) + 2.0 * (s[3] * s[3] + s[4] * s[4] + s[5] * s[5])
    scale = jnp.minimum(1.0, ALPHA0 * lax.rsqrt(size))
    return [scale * s[i] for i in range(6)]


def lanes(x, by):
    return x if by % 128 == 0 else pltpu.roll(x, by % 128, 1)


def subs(x, by):
    return pltpu.roll(x, by % 8, 0)


def flat(ref):
    fields, slabs, rows, columns = ref.shape
    return ref.reshape(fields, slabs * rows, columns)


def steps(ref, slab, row):
    return pl.ds(slab * ref.shape[2] + row, NZ, stride=ref.shape[2])


def line(ref, field, slab, row):
    return flat(ref)[field, steps(ref, slab, row), :]


def tile_iota(axis):
    return lax.broadcasted_iota(jnp.int32, (8, 128), axis)


def place(sizes):
    at = [lax.axis_index(n) for n in NAMES]
    return at, [at[i] < sizes[i] - 1 for i in range(3)], [at[i] > 0 for i in range(3)]


def primal_tile(z, t, masks, p, q, old, weight, below_x, above_x):
    first, last = masks[6], masks[7]
    rows = slice(8 + 8 * t, 16 + 8 * t)
    mine = slice(8 * t, 8 * t + 8)
    s = z * TILES + t
    pv = [p[c, z + 1, rows, :] for c in range(3)]
    div = masks[0] * pv[0] - jnp.where(first, lanes(below_x, -2 * s), lanes(pv[0], 1))
    div = div + ((masks[2] * pv[1] if t == TILES - 1 else pv[1]) - p[1, z + 1, 7 + 8 * t : 15 + 8 * t, :])
    div = div + ((masks[4] * pv[2] if z == NZ - 1 else pv[2]) - p[2, z, rows, :])
    fw, inverse = weight
    new = [(old[0] + TAU * div + fw) * inverse]
    bars = [2.0 * new[0] - old[0]]
    qv = [q[i, z, mine, :] for i in range(6)]
    qn = [jnp.where(last, lanes(above_x[j], 127 - 2 * s), lanes(qv[i], -1)) for j, i in enumerate(Q_OF[0])]
    for a in range(3):
        ix, iy, iz = Q_OF[a]
        total = pv[a] + (qn[a] - masks[1] * qv[ix])
        total = total + (q[iy, z, 1 + 8 * t : 9 + 8 * t, :] - (masks[3] * qv[iy] if t == 0 else qv[iy]))
        total = total + (q[iz, z + 1, mine, :] - (masks[5] * qv[iz] if z == 0 else qv[iz]))
        step = TAU * total
        new.append(old[1 + a] + step)
        bars.append(new[1 + a] + step)
    return new, bars


def edge_masks(up, down):
    lane, sub = tile_iota(1), tile_iota(0)
    first, last = lane == 0, lane == 127

    def at(where, inside):
        return jnp.where(jnp.logical_and(where, jnp.logical_not(inside)), 0.0, 1.0).astype(F32)

    return (at(last, up[0]), at(first, down[0]), at(sub == 7, up[1]), at(sub == 0, down[1]),
            jnp.where(up[2], 1.0, 0.0).astype(F32), jnp.where(down[2], 1.0, 0.0).astype(F32), first, last)


def exchange_kernel(sizes, f_in, w_in, u_in, v_in, p_in, q_in,
                    uv, p, q, fa, wb, cols,
                    bar0, bar1, bar2, xe, xey, xei, kept, xh_lo, xh_hi, d_xmyp, d_xpym, d_xmzp, d_xpzm,
                    pxk, qxk, plxk, quxk, plx, qux,
                    in_sem, send_sem, recv_sem):
    at, up, down = place(sizes)
    bars = (bar0, bar1, bar2)

    def exists(move):
        flag = None
        for i in range(3):
            if move[i]:
                one = up[i] if move[i] > 0 else down[i]
                flag = one if flag is None else jnp.logical_and(flag, one)
        return flag

    def device(move):
        return {NAMES[i]: at[i] + move[i] for i in range(3) if move[i]}

    def opposite(move):
        return tuple(-m for m in move)

    loads = [
        pltpu.make_async_copy(u_in, bar0.at[0, 1 : NZ + 1, 8 : 8 + NY, :], in_sem.at[0]),
        pltpu.make_async_copy(v_in, bar0.at[1:4, 1 : NZ + 1, 8 : 8 + NY, :], in_sem.at[1]),
        pltpu.make_async_copy(p_in, p.at[:, 1 : NZ + 1, 8 : 8 + NY, :], in_sem.at[2]),
        pltpu.make_async_copy(q_in, q.at[:, 0:NZ, 0:NY, :], in_sem.at[3]),
        pltpu.make_async_copy(f_in, fa, in_sem.at[4]),
        pltpu.make_async_copy(w_in, wb, in_sem.at[5]),
    ]
    barrier = pltpu.get_barrier_semaphore()
    arrivals = jnp.int32(0)
    for m in ALL:
        move = MOVES[m]
        arrivals = arrivals + exists(move).astype(jnp.int32)

        @pl.when(exists(move))
        def _():
            pl.semaphore_signal(
                barrier, inc=1, device_id=device(move), device_id_type=pl.DeviceIdType.MESH
            )

    for c in loads:
        c.start()

    def ends(m, r):
        bar = bars[r]
        inner = slice(1, NZ + 1)
        if m == ZUP:
            return bar.at[:, NZ, 8 : 8 + NY, :], bar.at[:, 0, 8 : 8 + NY, :]
        if m == ZDN:
            return bar.at[:, 1, 8 : 8 + NY, :], bar.at[:, NZ + 1, 8 : 8 + NY, :]
        if m == YUP:
            return bar.at[:, 1 : NZ + 1, 7 + NY, :], bar.at[:, 1 : NZ + 1, 7, :]
        if m == YDN:
            return bar.at[:, 1 : NZ + 1, 8, :], bar.at[:, 1 : NZ + 1, 8 + NY, :]
        if m == YUP_ZDN:
            return bar.at[:, 1, 7 + NY, :], bar.at[:, NZ + 1, 7, :]
        if m == YDN_ZUP:
            return bar.at[:, NZ, 8, :], bar.at[:, 0, 8 + NY, :]
        if m == PZ:
            return p_in.at[:, NZ - 1, :, :], p.at[:, 0, 8 : 8 + NY, :]
        if m == QZ:
            return q_in.at[:, 0, :, :], q.at[:, NZ, 0:NY, :]
        if m == PY:
            return p_in.at[:, :, NY - 1, :], p.at[:, 1 : NZ + 1, 7, :]
        if m == QY:
            return q_in.at[:, :, 0, :], q.at[:, 0:NZ, NY, :]
        if m == XUP_YDN:
            return xey.at[r, 0, :, 0, :], d_xmyp.at[r, :, 0, :]
        if m == XDN_YUP:
            return xey.at[r, 1, :, 7, :], d_xpym.at[r, :, 7, :]
        if m == PX_:
            return pxk, plxk
        if m == QX_:
            return qxk, quxk
        src, dst = {
            XUP: (xe, xh_lo), XDN: (xe, xh_hi),
            XUP_ZDN: (xe, d_xmzp), XDN_ZUP: (xe, d_xpzm),
        }[m]
        return src.at[r], dst.at[r]

    def message(m, r):
        src, dst = ends(m, r)
        return pltpu.make_async_remote_copy(
            src_ref=src, dst_ref=dst, send_sem=send_sem.at[r, m], recv_sem=recv_sem.at[r, m],
            device_id=device(MOVES[m]), device_id_type=pl.DeviceIdType.MESH,
        )

    def send(r, which):
        for m in which:
            @pl.when(exists(MOVES[m]))
            def _():
                message(m, r).start()

    def receive(r, which):
        for m in which:
            @pl.when(exists(opposite(MOVES[m])))
            def _():
                message(m, r).wait_recv()

    lane, sub = tile_iota(1), tile_iota(0)
    first, last = lane == 0, lane == 127
    edge = jnp.logical_or(first, last)
    zero = jnp.zeros((8, 128), F32)
    masks = edge_masks(up, down)

    def pack_into(acc, z, t, values, mask, by):
        for f, x in enumerate(values):
            acc[f // 2] = acc[f // 2] + lanes(jnp.where(mask, x, 0.0), (f % 2) * 64 + 2 * (z * TILES + t) + by)

    loads[0].wait()
    loads[1].wait()
    acc = [zero, zero]
    for t in OUTER + INNER:
        for z in range(NZ):
            pack_into(acc, z, t, [bar0[f, z + 1, 8 + 8 * t : 16 + 8 * t, :] for f in range(4)], edge, 0)
    for h in range(2):
        xe[0, h] = acc[h]
        xey[0, 0, h] = acc[h]
        xey[0, 1, h] = acc[h]
    loads[2].wait()
    loads[3].wait()
    accp, accq = [zero, zero], [zero, zero, zero]
    for t in EVERY:
        for z in range(NZ):
            pack_into(accp, z, t, [p[a, z + 1, 8 + 8 * t : 16 + 8 * t, :] for a in range(3)], last, 1)
            pack_into(accq, z, t, [q[i, z, 8 * t : 8 * t + 8, :] for i in range(6)], first, 0)
    for h in range(2):
        pxk[h] = accp[h]
    for h in range(3):
        qxk[h] = accq[h]

    pl.semaphore_wait(barrier, arrivals)
    send(0, ALL0)

    loads[4].wait()
    loads[5].wait()
    for z in range(NZ):
        for t in EVERY:
            rows = slice(8 * t, 8 * t + 8)
            tw = TAU * wb[z, rows, :]
            fa[z, rows, :] = tw * fa[z, rows, :]
            wb[z, rows, :] = 1.0 / (1.0 + tw)

    def split(x):
        return [x[0], lanes(x[0], 64), x[1], lanes(x[1], 64)]

    def clamp_x(r):
        @pl.when(jnp.logical_not(up[0]))
        def _():
            for h in range(2):
                xh_hi[r, h] = lanes(xe[r, h], 1)

        @pl.when(jnp.logical_not(down[0]))
        def _():
            for h in range(2):
                xh_lo[r, h] = lanes(xe[r, h], -1)

    def clamp_z(r):
        bar = bars[r]

        @pl.when(jnp.logical_not(up[2]))
        def _():
            bar[:, NZ + 1, 8 : 8 + NY, :] = bar[:, NZ, 8 : 8 + NY, :]

        @pl.when(jnp.logical_not(down[2]))
        def _():
            bar[:, 0, 8 : 8 + NY, :] = bar[:, 1, 8 : 8 + NY, :]

    def clamp_lower(r):
        bar = bars[r]

        @pl.when(jnp.logical_not(up[2]))
        def _():
            for f in range(4):
                bar[f, NZ + 1, 7:8, :] = bar[f, NZ, 7:8, :]

        @pl.when(jnp.logical_not(down[1]))
        def _():
            for f in range(4):
                bar[f, NZ + 1, 7:8, :] = bar[f, NZ + 1, 8:9, :]
                flat(bar)[f, steps(bar, 1, 7), :] = line(bar, f, 1, 8)

    def clamp_upper(r):
        bar = bars[r]

        @pl.when(jnp.logical_not(down[2]))
        def _():
            for f in range(4):
                bar[f, 0, 8 + NY : 9 + NY, :] = bar[f, 1, 8 + NY : 9 + NY, :]

        @pl.when(jnp.logical_not(up[1]))
        def _():
            for f in range(4):
                bar[f, 0, 8 + NY : 9 + NY, :] = bar[f, 0, 7 + NY : 8 + NY, :]
                flat(bar)[f, steps(bar, 1, 8 + NY), :] = line(bar, f, 1, 7 + NY)

    in64 = lax.rem(lane, 64)
    in8 = lax.rem(lane, 8)

    def x_below(r, corners):
        low = [lanes(xh_lo[r, h], 1) for h in range(2)]
        here = low[0]
        a = subs(here, -1)
        corner = jnp.where(up[1], lanes(subs(d_xmyp[r, 0], -1), 7), here) if corners else here
        ny = jnp.where(sub < 7, a, jnp.where(in8 < 6, lanes(a, -2), corner))
        nz = jnp.where(in64 < 56, lanes(here, -8), jnp.where(up[2], lanes(d_xmzp[r, 0], 57), here))
        new = p_step([plx[c] for c in range(3)], here, [xe[r, 0], ny, nz], split(low)[1:])
        if corners:
            for c in range(3):
                plx[c] = new[c]
        return jnp.where(down[0], new[0], zero)

    def x_above(r, corners):
        own_high = [lanes(xe[r, h], 1) for h in range(2)]
        high = [xh_hi[r, h] for h in range(2)]
        py_, pz_ = [], []
        for h in range(2):
            a = subs(high[h], 1)
            corner = jnp.where(down[1], lanes(subs(d_xpym[r, h], 1), -6), high[h]) if corners else high[h]
            py_.append(jnp.where(sub > 0, a, jnp.where(in8 >= 2, lanes(a, 2), corner)))
            pz_.append(jnp.where(in64 >= 8, lanes(high[h], 8),
                                 jnp.where(down[2], lanes(d_xpzm[r, h], -56), high[h])))
        new = q_step([qux[i] for i in range(6)], split(high)[1:],
                     [split(own_high)[1:], split(py_)[1:], split(pz_)[1:]])
        if corners:
            for i in range(6):
                qux[i] = new[i]
        return [jnp.where(up[0], new[i], zero) for i in Q_OF[0]]

    def high_column(source, f):
        row = jnp.broadcast_to(source[f // 2, 0:1, :], (8, 128))
        picked = jnp.where(lane == lax.rem(8 * sub + (f % 2) * 64 + 127, 128), row, 0.0)
        return jnp.broadcast_to(jnp.sum(picked, axis=1, keepdims=True), (8, 128))

    def low_column(source):
        row = jnp.broadcast_to(source[0, 7:8, :], (8, 128))
        return jnp.broadcast_to(jnp.sum(jnp.where(lane == 8 * sub + 6, row, 0.0), axis=1, keepdims=True), (8, 128))


    def keep_rows(r):
        for c in range(3):
            kept[c] = line(p, c, 1, 7 + NY)
            kept[10 + c] = high_column(xh_lo.at[r], 1 + c)
        for i in range(6):
            kept[3 + i] = line(q, i, 0, 0)
        kept[9] = low_column(xh_hi.at[r])

    def redo_upper(r):
        bar = bars[r]
        here = line(bar, 0, 1, 7 + NY)
        nx = jnp.where(last, kept[9], lanes(here, -1))
        new = p_step([kept[c] for c in range(3)], here, [nx, line(bar, 0, 1, 8 + NY), line(bar, 0, 2, 7 + NY)],
                     [line(bar, 1 + c, 1, 7 + NY) for c in range(3)])
        for c in range(3):
            flat(p)[c, steps(p, 1, 7 + NY), :] = new[c]

    def redo_lower(r):
        bar = bars[r]
        v = [line(bar, 1 + c, 1, 8) for c in range(3)]
        bx = [jnp.where(first, kept[10 + c], lanes(v[c], 1)) for c in range(3)]
        new = q_step([kept[3 + i] for i in range(6)], v,
                     [bx, [line(bar, 1 + c, 1, 7) for c in range(3)], [line(bar, 1 + c, 0, 8) for c in range(3)]])
        for i in range(6):
            flat(q)[i, steps(q, 0, 0), :] = new[i]

    def y_below(r):
        bar = bars[r]
        here = line(bar, 0, 1, 7)
        nx = jnp.where(lane < 127, lanes(here, -1), jnp.where(up[0], low_column(d_xpym.at[r]), here))
        new = p_step([line(p, c, 1, 7) for c in range(3)], here,
                     [nx, line(bar, 0, 1, 8), line(bar, 0, 2, 7)], [line(bar, 1 + c, 1, 7) for c in range(3)])
        new[1] = jnp.where(down[1], new[1], zero)
        for c in range(3):
            flat(p)[c, steps(p, 1, 7), :] = new[c]

    def y_above(r):
        bar = bars[r]
        v = [line(bar, 1 + c, 1, 8 + NY) for c in range(3)]
        bx = [jnp.where(lane > 0, lanes(v[c], 1), jnp.where(down[0], high_column(d_xmyp.at[r], 1 + c), v[c]))
              for c in range(3)]
        new = q_step([line(q, i, 0, NY) for i in range(6)], v,
                     [bx, [line(bar, 1 + c, 1, 7 + NY) for c in range(3)],
                      [line(bar, 1 + c, 0, 8 + NY) for c in range(3)]])
        for i in range(6):
            flat(q)[i, steps(q, 0, NY), :] = jnp.where(up[1], new[i], zero) if i in Q_OF[1] else new[i]

    def z_below(r, tiles):
        bar = bars[r]
        for t in tiles:
            rows = slice(8 + 8 * t, 16 + 8 * t)
            here = bar[0, 0, rows, :]
            nx = jnp.where(lane < 127, lanes(here, -1),
                           jnp.where(up[0], lanes(d_xpzm[r, 0], 127 - 56 - 2 * t), here))
            new = p_step([p[c, 0, rows, :] for c in range(3)], here,
                         [nx, bar[0, 0, 9 + 8 * t : 17 + 8 * t, :], bar[0, 1, rows, :]],
                         [bar[1 + c, 0, rows, :] for c in range(3)])
            new[2] = jnp.where(down[2], new[2], zero)
            for c in range(3):
                p[c, 0, rows, :] = new[c]

    def z_above(r, tiles):
        bar = bars[r]
        for t in tiles:
            rows = slice(8 + 8 * t, 16 + 8 * t)
            v = [bar[1 + c, NZ + 1, rows, :] for c in range(3)]
            bx = [jnp.where(lane > 0, lanes(v[c], 1),
                            jnp.where(down[0], lanes(d_xmzp[r, (1 + c) // 2], -((1 + c) % 2) * 64 - 2 * t + 1), v[c]))
                  for c in range(3)]
            new = q_step([q[i, NZ, 8 * t : 8 * t + 8, :] for i in range(6)], v,
                         [bx, [bar[1 + c, NZ + 1, 7 + 8 * t : 15 + 8 * t, :] for c in range(3)],
                          [bar[1 + c, NZ, rows, :] for c in range(3)]])
            for i in range(6):
                q[i, NZ, 8 * t : 8 * t + 8, :] = jnp.where(up[2], new[i], zero) if i in Q_OF[2] else new[i]

    def dual(r, slabs):
        bar = bars[r]
        high = xh_hi[r, 0]
        low = [xh_lo[r, h] for h in range(2)]
        for z in slabs:
            for t in EVERY:
                rows = slice(8 + 8 * t, 16 + 8 * t)
                mine = slice(8 * t, 8 * t + 8)
                s = z * TILES + t
                here = bar[0, z + 1, rows, :]
                v = [bar[1 + c, z + 1, rows, :] for c in range(3)]
                nx = jnp.where(last, lanes(high, 127 - 2 * s), lanes(here, -1))
                ny = subs(here, -1) if t == TILES - 1 else bar[0, z + 1, 9 + 8 * t : 17 + 8 * t, :]
                by = [subs(v[c], 1) if t == 0 else bar[1 + c, z + 1, 7 + 8 * t : 15 + 8 * t, :] for c in range(3)]
                new = p_step([p[c, z + 1, rows, :] for c in range(3)], here,
                             [nx, ny, bar[0, z + 2, rows, :]], v)
                for c in range(3):
                    p[c, z + 1, rows, :] = new[c]
                bx = [jnp.where(first, lanes(low[(1 + c) // 2], 1 - ((1 + c) % 2) * 64 - 2 * s), lanes(v[c], 1))
                      for c in range(3)]
                new = q_step([q[i, z, mine, :] for i in range(6)], v,
                             [bx, by, [bar[1 + c, z, rows, :] for c in range(3)]])
                for i in range(6):
                    q[i, z, mine, :] = new[i]

    def primal(r, tiles, acc, below_x, above_x):
        for t in tiles:
            for z in range(NZ):
                rows = slice(8 + 8 * t, 16 + 8 * t)
                mine = slice(8 * t, 8 * t + 8)
                if r == 0:
                    old = [bar0[f, z + 1, rows, :] for f in range(4)]
                else:
                    old = [uv[f, z, mine, :] for f in range(4)]
                new, values = primal_tile(z, t, masks, p, q, old, (fa[z, mine, :], wb[z, mine, :]), below_x, above_x)
                for f in range(4):
                    uv[f, z, mine, :] = new[f]
                    if r < ITERS - 1:
                        bars[r + 1][f, z + 1, rows, :] = values[f]
                if r < ITERS - 1:
                    pack_into(acc, z, t, values, edge, 0)

    low_side = at[1] < sizes[1] // 2
    for r in range(ITERS):
        start, more = r == 0, r < ITERS - 1
        receive(r, ALONG_X0 if start else ALONG_X)
        clamp_x(r)
        if start:
            for c in range(3):
                plx[c] = lanes(plxk[c // 2], (c % 2) * 64)
            for i in range(6):
                qux[i] = lanes(quxk[i // 2], (i % 2) * 64)
        keep_rows(r)
        dual(r, range(1, NZ - 1))
        receive(r, ALONG_Z0 if start else ALONG_Z)
        clamp_z(r)
        dual(r, (0, NZ - 1))
        z_below(r, EVERY[:-1])
        z_above(r, EVERY[1:])
        below_x, above_x = x_below(r, False), x_above(r, False)
        acc = [zero, zero]
        primal(r, INNER, acc, below_x, above_x)
        for h in range(2):
            xei[h] = acc[h]
        cols[0] = below_x
        for j in range(3):
            cols[1 + j] = above_x[j]

        def border(t, below, above, side, sends):
            acc = [zero, zero]
            primal(r, (t,), acc, below, above)
            for h in range(2):
                xey[r + 1, side, h] = acc[h]
            send(r + 1, sends)

        def lower():
            receive(r, LOWER0 if start else LOWER)
            clamp_lower(r)
            above = x_above(r, True)
            y_below(r)
            z_above(r, (0,))
            redo_lower(r)
            if more:
                border(0, cols[0], above, 0, UPPER)
            else:
                for j in range(3):
                    cols[4 + j] = above[j]

        def upper():
            receive(r, UPPER0 if start else UPPER)
            clamp_upper(r)
            below = x_below(r, True)
            y_above(r)
            z_below(r, (TILES - 1,))
            redo_upper(r)
            if more:
                border(TILES - 1, below, [cols[1 + j] for j in range(3)], 1, LOWER)
            else:
                cols[7] = below

        @pl.when(low_side)
        def _():
            lower()
            upper()

        @pl.when(jnp.logical_not(low_side))
        def _():
            upper()
            lower()

        if more:
            for h in range(2):
                xe[r + 1, h] = xei[h] + (xey[r + 1, 0, h] + xey[r + 1, 1, h])
            send(r + 1, ALONG_X + ALONG_Z)
    for r in range(ITERS):
        for m in (ALL0 if r == 0 else ALL):
            @pl.when(exists(MOVES[m]))
            def _():
                message(m, r).wait_send()


def final_kernel(sizes, uv, p, q, fa, wb, cols, u_out, v_out, p_out, q_out, new_uv, out_sem):
    _, up, down = place(sizes)
    masks = edge_masks(up, down)
    stores = [
        pltpu.make_async_copy(p.at[:, 1 : NZ + 1, 8 : 8 + NY, :], p_out, out_sem.at[0]),
        pltpu.make_async_copy(q.at[:, 0:NZ, 0:NY, :], q_out, out_sem.at[1]),
    ]
    for c in stores:
        c.start()
    middle = slice(8, NY - 8)
    more = [
        pltpu.make_async_copy(uv.at[0, :, middle, :], u_out.at[:, middle, :], out_sem.at[2]),
        pltpu.make_async_copy(uv.at[1:4, :, middle, :], v_out.at[:, :, middle, :], out_sem.at[3]),
    ]
    for c in more:
        c.start()
    stores += more
    for k, t in enumerate(OUTER):
        mine = slice(8 * t, 8 * t + 8)
        for z in range(NZ):
            new, _ = primal_tile(z, t, masks, p, q, [uv[f, z, mine, :] for f in range(4)],
                                 (fa[z, mine, :], wb[z, mine, :]), cols[7 * k],
                                 [cols[4 - 3 * k + j] for j in range(3)])
            for f in range(4):
                new_uv[k, f, z] = new[f]
        more = [
            pltpu.make_async_copy(new_uv.at[k, 0], u_out.at[:, mine, :], out_sem.at[4 + k]),
            pltpu.make_async_copy(new_uv.at[k, 1:4], v_out.at[:, :, mine, :], out_sem.at[6 + k]),
        ]
        for c in more:
            c.start()
        stores += more
    for c in stores:
        c.wait()


def per_device(sizes, *arrays):
    hbm = pl.BlockSpec(memory_space=pltpu.HBM)
    here = pl.BlockSpec(memory_space=pltpu.VMEM)
    tile = (8, 128)

    def vmem(*shape):
        return pltpu.VMEM(shape, F32)

    state = pl.pallas_call(
        functools.partial(exchange_kernel, sizes),
        out_shape=(
            vmem(4, NZ, NY, NX),
            vmem(3, NZ + 1, PROWS, NX),
            vmem(6, NZ + 1, PROWS, NX),
            vmem(NZ, NY, NX),
            vmem(NZ, NY, NX),
            vmem(8, *tile),
        ),
        in_specs=[hbm] * 6,
        out_specs=(here,) * 6,
        scratch_shapes=[
            vmem(4, NZ + 2, ROWS, NX), vmem(4, NZ + 2, ROWS, NX), vmem(4, NZ + 2, ROWS, NX),
            vmem(ITERS, 2, *tile), vmem(ITERS, 2, 2, *tile), vmem(2, *tile), vmem(13, *tile),
            vmem(ITERS, 2, *tile), vmem(ITERS, 2, *tile),
            vmem(ITERS, 2, *tile), vmem(ITERS, 2, *tile), vmem(ITERS, 2, *tile), vmem(ITERS, 2, *tile),
            vmem(2, *tile), vmem(3, *tile), vmem(2, *tile), vmem(3, *tile),
            vmem(3, *tile), vmem(6, *tile),
            pltpu.SemaphoreType.DMA((6,)),
            pltpu.SemaphoreType.DMA((ITERS, 18)),
            pltpu.SemaphoreType.DMA((ITERS, 18)),
        ],
        compiler_params=pltpu.CompilerParams(
            collective_id=0, has_side_effects=True, vmem_limit_bytes=24 << 20
        ),
        name="tgv_rounds",
    )(*[pltpu.with_memory_space_constraint(a, pltpu.HBM) for a in arrays])
    return pl.pallas_call(
        functools.partial(final_kernel, sizes),
        out_shape=tuple(jax.ShapeDtypeStruct(s, F32) for s in
                        ((NZ, NY, NX), (3, NZ, NY, NX), (3, NZ, NY, NX), (6, NZ, NY, NX))),
        in_specs=[here] * 6,
        out_specs=(hbm,) * 4,
        scratch_shapes=[vmem(2, 4, NZ, *tile), pltpu.SemaphoreType.DMA((8,))],
        compiler_params=pltpu.CompilerParams(vmem_limit_bytes=24 << 20),
        name="tgv_last",
    )(*state)


def solution(mesh):
    sizes = tuple(mesh.shape[n] for n in NAMES)
    scalar = P("gz", "gy", "gx")
    stack = P(None, "gz", "gy", "gx")
    return jax.shard_map(
        functools.partial(per_device, sizes), mesh=mesh,
        in_specs=(scalar, scalar, scalar, stack, stack, stack),
        out_specs=(scalar, stack, stack, stack), check_vma=False,
    )
```

```python
import functools

import jax
import jax.numpy as jnp
from jax import lax
from jax.experimental import pallas as pl
from jax.experimental.pallas import tpu as pltpu
from jax.sharding import PartitionSpec as P

ITERS = 3
SIGMA = 0.2
TAU = 0.2
ALPHA1 = 0.5
ALPHA0 = 1.0
NZ, NY, NX = 8, 32, 128
TILES = NY // 8
ROWS = NY + 16
PROWS = NY + 8
Q_OF = ((0, 3, 4), (3, 1, 5), (4, 5, 2))
F32 = jnp.float32
NAMES = ("gx", "gy", "gz")

(ZUP, ZDN, YUP, YDN, XUP, XDN, XUP_YDN, XDN_YUP, XUP_ZDN, XDN_ZUP, YUP_ZDN, YDN_ZUP,
 PZ, QZ, PY, QY, PX_, QX_) = range(18)
MOVES = {
    ZUP: (0, 0, 1), ZDN: (0, 0, -1), YUP: (0, 1, 0), YDN: (0, -1, 0), XUP: (1, 0, 0), XDN: (-1, 0, 0),
    XUP_YDN: (1, -1, 0), XDN_YUP: (-1, 1, 0), XUP_ZDN: (1, 0, -1), XDN_ZUP: (-1, 0, 1),
    YUP_ZDN: (0, 1, -1), YDN_ZUP: (0, -1, 1),
    PZ: (0, 0, 1), QZ: (0, 0, -1), PY: (0, 1, 0), QY: (0, -1, 0), PX_: (1, 0, 0), QX_: (-1, 0, 0),
}
N_BAR = 12
LOWER = (XDN_YUP, YUP, YUP_ZDN)
UPPER = (XUP_YDN, YDN, YDN_ZUP)
ALONG_X = (XUP, XDN)
ALONG_Z = (XUP_ZDN, XDN_ZUP, ZDN, ZUP)
LOWER0, UPPER0 = LOWER + (PY,), UPPER + (QY,)
ALONG_X0, ALONG_Z0 = ALONG_X + (PX_, QX_), ALONG_Z + (QZ, PZ)
ALL = LOWER + UPPER + ALONG_X + ALONG_Z
ALL0 = LOWER0 + UPPER0 + ALONG_X0 + ALONG_Z0
CORNER = (7, -6)
INNER = tuple(range(1, TILES - 1))
OUTER = (0, TILES - 1)
EVERY = tuple(range(TILES))


def p_step(p, here, following, v):
    t = [p[a] + SIGMA * ((following[a] - here) - v[a]) for a in range(3)]
    size = t[0] * t[0] + t[1] * t[1] + t[2] * t[2]
    scale = jnp.minimum(1.0, ALPHA1 * lax.rsqrt(size))
    return [scale * t[a] for a in range(3)]


def q_step(q, v, before):
    d = [[v[a] - before[b][a] for a in range(3)] for b in range(3)]
    s = [q[a] + SIGMA * d[a][a] for a in range(3)]
    s.append(q[3] + (0.5 * SIGMA) * (d[1][0] + d[0][1]))
    s.append(q[4] + (0.5 * SIGMA) * (d[2][0] + d[0][2]))
    s.append(q[5] + (0.5 * SIGMA) * (d[2][1] + d[1][2]))
    size = (s[0] * s[0] + s[1] * s[1] + s[2] * s[2]) + 2.0 * (s[3] * s[3] + s[4] * s[4] + s[5] * s[5])
    scale = jnp.minimum(1.0, ALPHA0 * lax.rsqrt(size))
    return [scale * s[i] for i in range(6)]


def lanes(x, by):
    return x if by % 128 == 0 else pltpu.roll(x, by % 128, 1)


def subs(x, by):
    return pltpu.roll(x, by % 8, 0)


def flat(ref):
    fields, slabs, rows, columns = ref.shape
    return ref.reshape(fields, slabs * rows, columns)


def steps(ref, slab, row):
    return pl.ds(slab * ref.shape[2] + row, NZ, stride=ref.shape[2])


def line(ref, field, slab, row):
    return flat(ref)[field, steps(ref, slab, row), :]


def tile_iota(axis):
    return lax.broadcasted_iota(jnp.int32, (8, 128), axis)


def place(sizes):
    at = [lax.axis_index(n) for n in NAMES]
    return at, [at[i] < sizes[i] - 1 for i in range(3)], [at[i] > 0 for i in range(3)]


def primal_tile(z, t, masks, p, q, old, weight, below_x, above_x):
    first, last = masks[6], masks[7]
    rows = slice(8 + 8 * t, 16 + 8 * t)
    mine = slice(8 * t, 8 * t + 8)
    s = z * TILES + t
    pv = [p[c, z + 1, rows, :] for c in range(3)]
    div = masks[0] * pv[0] - jnp.where(first, lanes(below_x, -2 * s), lanes(pv[0], 1))
    div = div + ((masks[2] * pv[1] if t == TILES - 1 else pv[1]) - p[1, z + 1, 7 + 8 * t : 15 + 8 * t, :])
    div = div + ((masks[4] * pv[2] if z == NZ - 1 else pv[2]) - p[2, z, rows, :])
    fw, inverse = weight
    new = [(old[0] + TAU * div + fw) * inverse]
    bars = [2.0 * new[0] - old[0]]
    qv = [q[i, z, mine, :] for i in range(6)]
    qn = [jnp.where(last, lanes(above_x[j], 127 - 2 * s), lanes(qv[i], -1)) for j, i in enumerate(Q_OF[0])]
    for a in range(3):
        ix, iy, iz = Q_OF[a]
        total = pv[a] + (qn[a] - masks[1] * qv[ix])
        total = total + (q[iy, z, 1 + 8 * t : 9 + 8 * t, :] - (masks[3] * qv[iy] if t == 0 else qv[iy]))
        total = total + (q[iz, z + 1, mine, :] - (masks[5] * qv[iz] if z == 0 else qv[iz]))
        step = TAU * total
        new.append(old[1 + a] + step)
        bars.append(new[1 + a] + step)
    return new, bars


def edge_masks(up, down):
    lane, sub = tile_iota(1), tile_iota(0)
    first, last = lane == 0, lane == 127

    def at(where, inside):
        return jnp.where(jnp.logical_and(where, jnp.logical_not(inside)), 0.0, 1.0).astype(F32)

    return (at(last, up[0]), at(first, down[0]), at(sub == 7, up[1]), at(sub == 0, down[1]),
            jnp.where(up[2], 1.0, 0.0).astype(F32), jnp.where(down[2], 1.0, 0.0).astype(F32), first, last)


def exchange_kernel(sizes, f_in, w_in, u_in, v_in, p_in, q_in,
                    uv, p, q, fa, wb, cols,
                    bar0, bar1, bar2, xe, xey, xei, kept, xh_lo, xh_hi, d_xmyp, d_xpym, d_xmzp, d_xpzm,
                    pxk, qxk, pyk, qyk, pzk, qzk, plxk, quxk, plx, qux,
                    in_sem, send_sem, recv_sem):
    at, up, down = place(sizes)
    bars = (bar0, bar1, bar2)

    def exists(move):
        flag = None
        for i in range(3):
            if move[i]:
                one = up[i] if move[i] > 0 else down[i]
                flag = one if flag is None else jnp.logical_and(flag, one)
        return flag

    def device(move):
        return {NAMES[i]: at[i] + move[i] for i in range(3) if move[i]}

    def opposite(move):
        return tuple(-m for m in move)

    loads = [
        pltpu.make_async_copy(u_in, bar0.at[0, 1 : NZ + 1, 8 : 8 + NY, :], in_sem.at[0]),
        pltpu.make_async_copy(v_in, bar0.at[1:4, 1 : NZ + 1, 8 : 8 + NY, :], in_sem.at[1]),
        pltpu.make_async_copy(p_in, p.at[:, 1 : NZ + 1, 8 : 8 + NY, :], in_sem.at[2]),
        pltpu.make_async_copy(q_in, q.at[:, 0:NZ, 0:NY, :], in_sem.at[3]),
        pltpu.make_async_copy(f_in, fa, in_sem.at[4]),
        pltpu.make_async_copy(w_in, wb, in_sem.at[5]),
    ]
    barrier = pltpu.get_barrier_semaphore()
    arrivals = jnp.int32(0)
    for m in ALL:
        move = MOVES[m]
        arrivals = arrivals + exists(move).astype(jnp.int32)

        @pl.when(exists(move))
        def _():
            pl.semaphore_signal(
                barrier, inc=1, device_id=device(move), device_id_type=pl.DeviceIdType.MESH
            )

    for c in loads:
        c.start()

    def ends(m, r):
        bar = bars[r]
        inner = slice(1, NZ + 1)
        if m == ZUP:
            return bar.at[:, NZ, 8 : 8 + NY, :], bar.at[:, 0, 8 : 8 + NY, :]
        if m == ZDN:
            return bar.at[:, 1, 8 : 8 + NY, :], bar.at[:, NZ + 1, 8 : 8 + NY, :]
        if m == YUP:
            return bar.at[:, 1 : NZ + 1, 7 + NY, :], bar.at[:, 1 : NZ + 1, 7, :]
        if m == YDN:
            return bar.at[:, 1 : NZ + 1, 8, :], bar.at[:, 1 : NZ + 1, 8 + NY, :]
        if m == YUP_ZDN:
            return bar.at[:, 1, 7 + NY, :], bar.at[:, NZ + 1, 7, :]
        if m == YDN_ZUP:
            return bar.at[:, NZ, 8, :], bar.at[:, 0, 8 + NY, :]
        if m == PZ:
            return pzk, p.at[:, 0, 8 : 8 + NY, :]
        if m == QZ:
            return qzk, q.at[:, NZ, 0:NY, :]
        if m == PY:
            return pyk, p.at[:, 1 : NZ + 1, 7, :]
        if m == QY:
            return qyk, q.at[:, 0:NZ, NY, :]
        if m == XUP_YDN:
            return xey.at[r, 0, :, 0, :], d_xmyp.at[r, :, 7, :]
        if m == XDN_YUP:
            return xey.at[r, 1, :, 7, :], d_xpym.at[r, :, 0, :]
        if m == PX_:
            return pxk, plxk
        if m == QX_:
            return qxk, quxk
        src, dst = {
            XUP: (xe, xh_lo), XDN: (xe, xh_hi),
            XUP_ZDN: (xe, d_xmzp), XDN_ZUP: (xe, d_xpzm),
        }[m]
        return src.at[r], dst.at[r]

    def message(m, r):
        src, dst = ends(m, r)
        return pltpu.make_async_remote_copy(
            src_ref=src, dst_ref=dst, send_sem=send_sem.at[r, m], recv_sem=recv_sem.at[r, m],
            device_id=device(MOVES[m]), device_id_type=pl.DeviceIdType.MESH,
        )

    def send(r, which):
        for m in which:
            @pl.when(exists(MOVES[m]))
            def _():
                message(m, r).start()

    def sent(r):
        for m in ALL0 if r == 0 else ALL:
            @pl.when(exists(MOVES[m]))
            def _():
                message(m, r).wait_send()

    def receive(r, which):
        for m in which:
            @pl.when(exists(opposite(MOVES[m])))
            def _():
                message(m, r).wait_recv()

    lane, sub = tile_iota(1), tile_iota(0)
    first, last = lane == 0, lane == 127
    edge = jnp.logical_or(first, last)
    zero = jnp.zeros((8, 128), F32)
    masks = edge_masks(up, down)

    def pack_into(acc, z, t, values, mask, by):
        for f, x in enumerate(values):
            acc[f // 2] = acc[f // 2] + lanes(jnp.where(mask, x, 0.0), (f % 2) * 64 + 2 * (z * TILES + t) + by)

    loads[0].wait()
    loads[1].wait()
    acc = [zero, zero]
    for t in OUTER + INNER:
        for z in range(NZ):
            pack_into(acc, z, t, [bar0[f, z + 1, 8 + 8 * t : 16 + 8 * t, :] for f in range(4)], edge, 0)
    for h in range(2):
        xe[0, h] = acc[h]
        xey[0, 0, h] = lanes(acc[h], CORNER[0])
        xey[0, 1, h] = lanes(acc[h], CORNER[1])
    loads[2].wait()
    loads[3].wait()
    for c in range(3):
        pyk[c] = line(p, c, 1, 7 + NY)
        pzk[c] = p[c, NZ, 8 : 8 + NY, :]
    for i in range(6):
        qyk[i] = line(q, i, 0, 0)
        qzk[i] = q[i, 0, 0:NY, :]
    accp, accq = [zero, zero], [zero, zero, zero]
    for t in EVERY:
        for z in range(NZ):
            pack_into(accp, z, t, [p[a, z + 1, 8 + 8 * t : 16 + 8 * t, :] for a in range(3)], last, 1)
            pack_into(accq, z, t, [q[i, z, 8 * t : 8 * t + 8, :] for i in range(6)], first, 0)
    for h in range(2):
        pxk[h] = accp[h]
    for h in range(3):
        qxk[h] = accq[h]

    pl.semaphore_wait(barrier, arrivals)
    send(0, ALL0)

    loads[4].wait()
    loads[5].wait()
    for z in range(NZ):
        for t in EVERY:
            rows = slice(8 * t, 8 * t + 8)
            tw = TAU * wb[z, rows, :]
            fa[z, rows, :] = tw * fa[z, rows, :]
            wb[z, rows, :] = 1.0 / (1.0 + tw)

    def split(x):
        return [x[0], lanes(x[0], 64), x[1], lanes(x[1], 64)]

    def clamp_x(r):
        @pl.when(jnp.logical_not(up[0]))
        def _():
            for h in range(2):
                xh_hi[r, h] = lanes(xe[r, h], 1)

        @pl.when(jnp.logical_not(down[0]))
        def _():
            for h in range(2):
                xh_lo[r, h] = lanes(xe[r, h], -1)

    def clamp_z(r):
        bar = bars[r]

        @pl.when(jnp.logical_not(up[2]))
        def _():
            bar[:, NZ + 1, 8 : 8 + NY, :] = bar[:, NZ, 8 : 8 + NY, :]

        @pl.when(jnp.logical_not(down[2]))
        def _():
            bar[:, 0, 8 : 8 + NY, :] = bar[:, 1, 8 : 8 + NY, :]

    def clamp_lower(r):
        bar = bars[r]

        @pl.when(jnp.logical_not(up[2]))
        def _():
            for f in range(4):
                bar[f, NZ + 1, 7:8, :] = bar[f, NZ, 7:8, :]

        @pl.when(jnp.logical_not(down[1]))
        def _():
            for f in range(4):
                bar[f, NZ + 1, 7:8, :] = bar[f, NZ + 1, 8:9, :]
                flat(bar)[f, steps(bar, 1, 7), :] = line(bar, f, 1, 8)

    def clamp_upper(r):
        bar = bars[r]

        @pl.when(jnp.logical_not(down[2]))
        def _():
            for f in range(4):
                bar[f, 0, 8 + NY : 9 + NY, :] = bar[f, 1, 8 + NY : 9 + NY, :]

        @pl.when(jnp.logical_not(up[1]))
        def _():
            for f in range(4):
                bar[f, 0, 8 + NY : 9 + NY, :] = bar[f, 0, 7 + NY : 8 + NY, :]
                flat(bar)[f, steps(bar, 1, 8 + NY), :] = line(bar, f, 1, 7 + NY)

    in64 = lax.rem(lane, 64)
    in8 = lax.rem(lane, 8)

    def x_below(r, corners):
        low = [lanes(xh_lo[r, h], 1) for h in range(2)]
        here = low[0]
        a = subs(here, -1)
        corner = jnp.where(up[1], d_xmyp[r, 0], here) if corners else here
        ny = jnp.where(sub < 7, a, jnp.where(in8 < 6, lanes(a, -2), corner))
        nz = jnp.where(in64 < 56, lanes(here, -8), jnp.where(up[2], lanes(d_xmzp[r, 0], 57), here))
        new = p_step([plx[c] for c in range(3)], here, [xe[r, 0], ny, nz], split(low)[1:])
        if corners:
            for c in range(3):
                plx[c] = new[c]
        return jnp.where(down[0], new[0], zero)

    def x_above(r, corners):
        own_high = [lanes(xe[r, h], 1) for h in range(2)]
        high = [xh_hi[r, h] for h in range(2)]
        py_, pz_ = [], []
        for h in range(2):
            a = subs(high[h], 1)
            corner = jnp.where(down[1], d_xpym[r, h], high[h]) if corners else high[h]
            py_.append(jnp.where(sub > 0, a, jnp.where(in8 >= 2, lanes(a, 2), corner)))
            pz_.append(jnp.where(in64 >= 8, lanes(high[h], 8),
                                 jnp.where(down[2], lanes(d_xpzm[r, h], -56), high[h])))
        new = q_step([qux[i] for i in range(6)], split(high)[1:],
                     [split(own_high)[1:], split(py_)[1:], split(pz_)[1:]])
        if corners:
            for i in range(6):
                qux[i] = new[i]
        return [jnp.where(up[0], new[i], zero) for i in Q_OF[0]]

    def column(source, row, base):
        line_ = jnp.broadcast_to(source[row : row + 1, :], (8, 128))
        picked = jnp.where(lane == lax.rem(8 * sub + base % 128, 128), line_, 0.0)
        return jnp.broadcast_to(jnp.sum(picked, axis=1, keepdims=True), (8, 128))

    def keep_rows(r):
        for c in range(3):
            kept[c] = line(p, c, 1, 7 + NY)
            kept[10 + c] = column(xh_lo.at[r, (1 + c) // 2], 0, ((1 + c) % 2) * 64 - 1)
        for i in range(6):
            kept[3 + i] = line(q, i, 0, 0)
        kept[9] = column(xh_hi.at[r, 0], 7, 6)

    def redo_upper(r):
        bar = bars[r]
        here = line(bar, 0, 1, 7 + NY)
        nx = jnp.where(last, kept[9], lanes(here, -1))
        new = p_step([kept[c] for c in range(3)], here, [nx, line(bar, 0, 1, 8 + NY), line(bar, 0, 2, 7 + NY)],
                     [line(bar, 1 + c, 1, 7 + NY) for c in range(3)])
        for c in range(3):
            flat(p)[c, steps(p, 1, 7 + NY), :] = new[c]

    def redo_lower(r):
        bar = bars[r]
        v = [line(bar, 1 + c, 1, 8) for c in range(3)]
        bx = [jnp.where(first, kept[10 + c], lanes(v[c], 1)) for c in range(3)]
        new = q_step([kept[3 + i] for i in range(6)], v,
                     [bx, [line(bar, 1 + c, 1, 7) for c in range(3)], [line(bar, 1 + c, 0, 8) for c in range(3)]])
        for i in range(6):
            flat(q)[i, steps(q, 0, 0), :] = new[i]

    def y_below(r):
        bar = bars[r]
        here = line(bar, 0, 1, 7)
        nx = jnp.where(lane < 127, lanes(here, -1), jnp.where(up[0], column(d_xpym.at[r, 0], 0, 6 + CORNER[1]), here))
        new = p_step([line(p, c, 1, 7) for c in range(3)], here,
                     [nx, line(bar, 0, 1, 8), line(bar, 0, 2, 7)], [line(bar, 1 + c, 1, 7) for c in range(3)])
        new[1] = jnp.where(down[1], new[1], zero)
        for c in range(3):
            flat(p)[c, steps(p, 1, 7), :] = new[c]

    def y_above(r):
        bar = bars[r]
        v = [line(bar, 1 + c, 1, 8 + NY) for c in range(3)]
        bx = [jnp.where(lane > 0, lanes(v[c], 1), jnp.where(down[0], column(d_xmyp.at[r, (1 + c) // 2], 7, ((1 + c) % 2) * 64 - 1 + CORNER[0]), v[c]))
              for c in range(3)]
        new = q_step([line(q, i, 0, NY) for i in range(6)], v,
                     [bx, [line(bar, 1 + c, 1, 7 + NY) for c in range(3)],
                      [line(bar, 1 + c, 0, 8 + NY) for c in range(3)]])
        for i in range(6):
            flat(q)[i, steps(q, 0, NY), :] = jnp.where(up[1], new[i], zero) if i in Q_OF[1] else new[i]

    def z_below(r, tiles):
        bar = bars[r]
        for t in tiles:
            rows = slice(8 + 8 * t, 16 + 8 * t)
            here = bar[0, 0, rows, :]
            nx = jnp.where(lane < 127, lanes(here, -1),
                           jnp.where(up[0], lanes(d_xpzm[r, 0], 127 - 56 - 2 * t), here))
            new = p_step([p[c, 0, rows, :] for c in range(3)], here,
                         [nx, bar[0, 0, 9 + 8 * t : 17 + 8 * t, :], bar[0, 1, rows, :]],
                         [bar[1 + c, 0, rows, :] for c in range(3)])
            new[2] = jnp.where(down[2], new[2], zero)
            for c in range(3):
                p[c, 0, rows, :] = new[c]

    def z_above(r, tiles):
        bar = bars[r]
        for t in tiles:
            rows = slice(8 + 8 * t, 16 + 8 * t)
            v = [bar[1 + c, NZ + 1, rows, :] for c in range(3)]
            bx = [jnp.where(lane > 0, lanes(v[c], 1),
                            jnp.where(down[0], lanes(d_xmzp[r, (1 + c) // 2], -((1 + c) % 2) * 64 - 2 * t + 1), v[c]))
                  for c in range(3)]
            new = q_step([q[i, NZ, 8 * t : 8 * t + 8, :] for i in range(6)], v,
                         [bx, [bar[1 + c, NZ + 1, 7 + 8 * t : 15 + 8 * t, :] for c in range(3)],
                          [bar[1 + c, NZ, rows, :] for c in range(3)]])
            for i in range(6):
                q[i, NZ, 8 * t : 8 * t + 8, :] = jnp.where(up[2], new[i], zero) if i in Q_OF[2] else new[i]

    def dual(r, slabs):
        bar = bars[r]
        high = xh_hi[r, 0]
        low = [xh_lo[r, h] for h in range(2)]
        for z in slabs:
            for t in EVERY:
                rows = slice(8 + 8 * t, 16 + 8 * t)
                mine = slice(8 * t, 8 * t + 8)
                s = z * TILES + t
                here = bar[0, z + 1, rows, :]
                v = [bar[1 + c, z + 1, rows, :] for c in range(3)]
                nx = jnp.where(last, lanes(high, 127 - 2 * s), lanes(here, -1))
                ny = subs(here, -1) if t == TILES - 1 else bar[0, z + 1, 9 + 8 * t : 17 + 8 * t, :]
                by = [subs(v[c], 1) if t == 0 else bar[1 + c, z + 1, 7 + 8 * t : 15 + 8 * t, :] for c in range(3)]
                new = p_step([p[c, z + 1, rows, :] for c in range(3)], here,
                             [nx, ny, bar[0, z + 2, rows, :]], v)
                for c in range(3):
                    p[c, z + 1, rows, :] = new[c]
                bx = [jnp.where(first, lanes(low[(1 + c) // 2], 1 - ((1 + c) % 2) * 64 - 2 * s), lanes(v[c], 1))
                      for c in range(3)]
                new = q_step([q[i, z, mine, :] for i in range(6)], v,
                             [bx, by, [bar[1 + c, z, rows, :] for c in range(3)]])
                for i in range(6):
                    q[i, z, mine, :] = new[i]

    def primal(r, tiles, acc, below_x, above_x, by=0):
        for t in tiles:
            for z in range(NZ):
                rows = slice(8 + 8 * t, 16 + 8 * t)
                mine = slice(8 * t, 8 * t + 8)
                if r == 0:
                    old = [bar0[f, z + 1, rows, :] for f in range(4)]
                else:
                    old = [uv[f, z, mine, :] for f in range(4)]
                new, values = primal_tile(z, t, masks, p, q, old, (fa[z, mine, :], wb[z, mine, :]), below_x, above_x)
                for f in range(4):
                    uv[f, z, mine, :] = new[f]
                    if r < ITERS - 1:
                        bars[r + 1][f, z + 1, rows, :] = values[f]
                if r < ITERS - 1:
                    pack_into(acc, z, t, values, edge, by)

    low_side = at[1] < sizes[1] // 2
    for r in range(ITERS):
        start, more = r == 0, r < ITERS - 1
        receive(r, ALONG_X0 if start else ALONG_X)
        clamp_x(r)
        if start:
            for c in range(3):
                plx[c] = lanes(plxk[c // 2], (c % 2) * 64)
            for i in range(6):
                qux[i] = lanes(quxk[i // 2], (i % 2) * 64)
        keep_rows(r)
        dual(r, range(1, NZ - 1))
        receive(r, ALONG_Z0 if start else ALONG_Z)
        clamp_z(r)
        dual(r, (0, NZ - 1))
        z_below(r, EVERY[:-1])
        z_above(r, EVERY[1:])
        below_x, above_x = x_below(r, False), x_above(r, False)
        acc = [zero, zero]
        primal(r, INNER, acc, below_x, above_x)
        if r > 0:
            sent(r - 1)
        for h in range(2):
            xei[h] = acc[h]
        cols[0] = below_x
        for j in range(3):
            cols[1 + j] = above_x[j]

        def border(t, below, above, side, sends):
            acc = [zero, zero]
            primal(r, (t,), acc, below, above, CORNER[side])
            for h in range(2):
                xey[r + 1, side, h] = acc[h]
            send(r + 1, sends)

        def lower():
            receive(r, LOWER0 if start else LOWER)
            clamp_lower(r)
            above = x_above(r, True)
            y_below(r)
            z_above(r, (0,))
            redo_lower(r)
            if more:
                border(0, cols[0], above, 0, UPPER)
            else:
                for j in range(3):
                    cols[4 + j] = above[j]

        def upper():
            receive(r, UPPER0 if start else UPPER)
            clamp_upper(r)
            below = x_below(r, True)
            y_above(r)
            z_below(r, (TILES - 1,))
            redo_upper(r)
            if more:
                border(TILES - 1, below, [cols[1 + j] for j in range(3)], 1, LOWER)
            else:
                cols[7] = below

        @pl.when(low_side)
        def _():
            lower()
            upper()

        @pl.when(jnp.logical_not(low_side))
        def _():
            upper()
            lower()

        if more:
            for h in range(2):
                xe[r + 1, h] = xei[h] + (lanes(xey[r + 1, 0, h], -CORNER[0]) + lanes(xey[r + 1, 1, h], -CORNER[1]))
            send(r + 1, ALONG_X + ALONG_Z)
    sent(ITERS - 1)


def final_kernel(sizes, uv, p, q, fa, wb, cols, u_out, v_out, p_out, q_out, new_uv, out_sem):
    _, up, down = place(sizes)
    masks = edge_masks(up, down)
    stores = [
        pltpu.make_async_copy(p.at[:, 1 : NZ + 1, 8 : 8 + NY, :], p_out, out_sem.at[0]),
        pltpu.make_async_copy(q.at[:, 0:NZ, 0:NY, :], q_out, out_sem.at[1]),
    ]
    for c in stores:
        c.start()
    middle = slice(8, NY - 8)
    more = [
        pltpu.make_async_copy(uv.at[0, :, middle, :], u_out.at[:, middle, :], out_sem.at[2]),
        pltpu.make_async_copy(uv.at[1:4, :, middle, :], v_out.at[:, :, middle, :], out_sem.at[3]),
    ]
    for c in more:
        c.start()
    stores += more
    for k, t in enumerate(OUTER):
        mine = slice(8 * t, 8 * t + 8)
        for z in range(NZ):
            new, _ = primal_tile(z, t, masks, p, q, [uv[f, z, mine, :] for f in range(4)],
                                 (fa[z, mine, :], wb[z, mine, :]), cols[7 * k],
                                 [cols[4 - 3 * k + j] for j in range(3)])
            for f in range(4):
                new_uv[k, f, z] = new[f]
        more = [
            pltpu.make_async_copy(new_uv.at[k, 0], u_out.at[:, mine, :], out_sem.at[4 + k]),
            pltpu.make_async_copy(new_uv.at[k, 1:4], v_out.at[:, :, mine, :], out_sem.at[6 + k]),
        ]
        for c in more:
            c.start()
        stores += more
    for c in stores:
        c.wait()


def per_device(sizes, *arrays):
    hbm = pl.BlockSpec(memory_space=pltpu.HBM)
    here = pl.BlockSpec(memory_space=pltpu.VMEM)
    tile = (8, 128)

    def vmem(*shape):
        return pltpu.VMEM(shape, F32)

    state = pl.pallas_call(
        functools.partial(exchange_kernel, sizes),
        out_shape=(
            vmem(4, NZ, NY, NX),
            vmem(3, NZ + 1, PROWS, NX),
            vmem(6, NZ + 1, PROWS, NX),
            vmem(NZ, NY, NX),
            vmem(NZ, NY, NX),
            vmem(8, *tile),
        ),
        in_specs=[hbm] * 6,
        out_specs=(here,) * 6,
        scratch_shapes=[
            vmem(4, NZ + 2, ROWS, NX), vmem(4, NZ + 2, ROWS, NX), vmem(4, NZ + 2, ROWS, NX),
            vmem(ITERS, 2, *tile), vmem(ITERS, 2, 2, *tile), vmem(2, *tile), vmem(13, *tile),
            vmem(ITERS, 2, *tile), vmem(ITERS, 2, *tile),
            vmem(ITERS, 2, *tile), vmem(ITERS, 2, *tile), vmem(ITERS, 2, *tile), vmem(ITERS, 2, *tile),
            vmem(2, *tile), vmem(3, *tile), vmem(3, *tile), vmem(6, *tile), vmem(3, NY, NX), vmem(6, NY, NX),
            vmem(2, *tile), vmem(3, *tile),
            vmem(3, *tile), vmem(6, *tile),
            pltpu.SemaphoreType.DMA((6,)),
            pltpu.SemaphoreType.DMA((ITERS, 18)),
            pltpu.SemaphoreType.DMA((ITERS, 18)),
        ],
        compiler_params=pltpu.CompilerParams(
            collective_id=0, has_side_effects=True, vmem_limit_bytes=24 << 20
        ),
        name="tgv_rounds",
    )(*[pltpu.with_memory_space_constraint(a, pltpu.HBM) for a in arrays])
    return pl.pallas_call(
        functools.partial(final_kernel, sizes),
        out_shape=tuple(jax.ShapeDtypeStruct(s, F32) for s in
                        ((NZ, NY, NX), (3, NZ, NY, NX), (3, NZ, NY, NX), (6, NZ, NY, NX))),
        in_specs=[here] * 6,
        out_specs=(hbm,) * 4,
        scratch_shapes=[vmem(2, 4, NZ, *tile), pltpu.SemaphoreType.DMA((8,))],
        compiler_params=pltpu.CompilerParams(vmem_limit_bytes=24 << 20),
        name="tgv_last",
    )(*state)


def solution(mesh):
    sizes = tuple(mesh.shape[n] for n in NAMES)
    scalar = P("gz", "gy", "gx")
    stack = P(None, "gz", "gy", "gx")
    return jax.shard_map(
        functools.partial(per_device, sizes), mesh=mesh,
        in_specs=(scalar, scalar, scalar, stack, stack, stack),
        out_specs=(scalar, stack, stack, stack), check_vma=False,
    )
```

```python
import functools

import jax
import jax.numpy as jnp
from jax import lax
from jax.experimental import pallas as pl
from jax.experimental.pallas import tpu as pltpu
from jax.sharding import PartitionSpec as P

ITERS = 3
SIGMA = 0.2
TAU = 0.2
ALPHA1 = 0.5
ALPHA0 = 1.0
NZ, NY, NX = 8, 32, 128
TILES = NY // 8
ROWS = NY + 16
PROWS = NY + 8
Q_OF = ((0, 3, 4), (3, 1, 5), (4, 5, 2))
F32 = jnp.float32
NAMES = ("gx", "gy", "gz")

(ZUP, ZDN, YUP, YDN, XUP, XDN, XUP_YDN, XDN_YUP, XUP_ZDN, XDN_ZUP, YUP_ZDN, YDN_ZUP,
 PZ, QZ, PY, QY, PX_, QX_) = range(18)
MOVES = {
    ZUP: (0, 0, 1), ZDN: (0, 0, -1), YUP: (0, 1, 0), YDN: (0, -1, 0), XUP: (1, 0, 0), XDN: (-1, 0, 0),
    XUP_YDN: (1, -1, 0), XDN_YUP: (-1, 1, 0), XUP_ZDN: (1, 0, -1), XDN_ZUP: (-1, 0, 1),
    YUP_ZDN: (0, 1, -1), YDN_ZUP: (0, -1, 1),
    PZ: (0, 0, 1), QZ: (0, 0, -1), PY: (0, 1, 0), QY: (0, -1, 0), PX_: (1, 0, 0), QX_: (-1, 0, 0),
}
N_BAR = 12
LOWER = (XDN_YUP, YUP, YUP_ZDN)
UPPER = (XUP_YDN, YDN, YDN_ZUP)
ALONG_X = (XUP, XDN)
ALONG_Z = (XUP_ZDN, XDN_ZUP, ZDN, ZUP)
LOWER0, UPPER0 = LOWER + (PY,), UPPER + (QY,)
ALONG_X0, ALONG_Z0 = ALONG_X + (PX_, QX_), ALONG_Z + (QZ, PZ)
ALL = LOWER + UPPER + ALONG_X + ALONG_Z
ALL0 = LOWER0 + UPPER0 + ALONG_X0 + ALONG_Z0
CORNER = (7, -6)
INNER = tuple(range(1, TILES - 1))
OUTER = (0, TILES - 1)
EVERY = tuple(range(TILES))


def p_step(p, here, following, v):
    t = [p[a] + SIGMA * ((following[a] - here) - v[a]) for a in range(3)]
    size = t[0] * t[0] + t[1] * t[1] + t[2] * t[2]
    scale = jnp.minimum(1.0, ALPHA1 * lax.rsqrt(size))
    return [scale * t[a] for a in range(3)]


def q_step(q, v, before):
    d = [[v[a] - before[b][a] for a in range(3)] for b in range(3)]
    s = [q[a] + SIGMA * d[a][a] for a in range(3)]
    s.append(q[3] + (0.5 * SIGMA) * (d[1][0] + d[0][1]))
    s.append(q[4] + (0.5 * SIGMA) * (d[2][0] + d[0][2]))
    s.append(q[5] + (0.5 * SIGMA) * (d[2][1] + d[1][2]))
    size = (s[0] * s[0] + s[1] * s[1] + s[2] * s[2]) + 2.0 * (s[3] * s[3] + s[4] * s[4] + s[5] * s[5])
    scale = jnp.minimum(1.0, ALPHA0 * lax.rsqrt(size))
    return [scale * s[i] for i in range(6)]


def lanes(x, by):
    return x if by % 128 == 0 else pltpu.roll(x, by % 128, 1)


def subs(x, by):
    return pltpu.roll(x, by % 8, 0)


def flat(ref):
    fields, slabs, rows, columns = ref.shape
    return ref.reshape(fields, slabs * rows, columns)


def steps(ref, slab, row):
    return pl.ds(slab * ref.shape[2] + row, NZ, stride=ref.shape[2])


def line(ref, field, slab, row):
    return flat(ref)[field, steps(ref, slab, row), :]


def tile_iota(axis):
    return lax.broadcasted_iota(jnp.int32, (8, 128), axis)


def place(sizes):
    at = [lax.axis_index(n) for n in NAMES]
    return at, [at[i] < sizes[i] - 1 for i in range(3)], [at[i] > 0 for i in range(3)]


def primal_tile(z, t, masks, p, q, old, weight, below_x, above_x):
    first, last = masks[6], masks[7]
    rows = slice(8 + 8 * t, 16 + 8 * t)
    mine = slice(8 * t, 8 * t + 8)
    s = z * TILES + t
    pv = [p[c, z + 1, rows, :] for c in range(3)]
    div = masks[0] * pv[0] - jnp.where(first, lanes(below_x, -2 * s), lanes(pv[0], 1))
    div = div + ((masks[2] * pv[1] if t == TILES - 1 else pv[1]) - p[1, z + 1, 7 + 8 * t : 15 + 8 * t, :])
    div = div + ((masks[4] * pv[2] if z == NZ - 1 else pv[2]) - p[2, z, rows, :])
    fw, inverse = weight
    new = [(old[0] + TAU * div + fw) * inverse]
    bars = [2.0 * new[0] - old[0]]
    qv = [q[i, z, mine, :] for i in range(6)]
    qn = [jnp.where(last, lanes(above_x[j], 127 - 2 * s), lanes(qv[i], -1)) for j, i in enumerate(Q_OF[0])]
    for a in range(3):
        ix, iy, iz = Q_OF[a]
        total = pv[a] + (qn[a] - masks[1] * qv[ix])
        total = total + (q[iy, z, 1 + 8 * t : 9 + 8 * t, :] - (masks[3] * qv[iy] if t == 0 else qv[iy]))
        total = total + (q[iz, z + 1, mine, :] - (masks[5] * qv[iz] if z == 0 else qv[iz]))
        step = TAU * total
        new.append(old[1 + a] + step)
        bars.append(new[1 + a] + step)
    return new, bars


def edge_masks(up, down):
    lane, sub = tile_iota(1), tile_iota(0)
    first, last = lane == 0, lane == 127

    def at(where, inside):
        return jnp.where(jnp.logical_and(where, jnp.logical_not(inside)), 0.0, 1.0).astype(F32)

    return (at(last, up[0]), at(first, down[0]), at(sub == 7, up[1]), at(sub == 0, down[1]),
            jnp.where(up[2], 1.0, 0.0).astype(F32), jnp.where(down[2], 1.0, 0.0).astype(F32), first, last)


def exchange_kernel(sizes, f_in, w_in, u_in, v_in, p_in, q_in,
                    uv, p, q, fa, wb, cols,
                    bar0, bar1, bar2, xe, xey, xei, kept, early, xh_lo, xh_hi, d_xmyp, d_xpym, d_xmzp, d_xpzm,
                    pxk, qxk, pyk, qyk, pzk, qzk, plxk, quxk, plx, qux,
                    in_sem, send_sem, recv_sem):
    at, up, down = place(sizes)
    bars = (bar0, bar1, bar2)

    def exists(move):
        flag = None
        for i in range(3):
            if move[i]:
                one = up[i] if move[i] > 0 else down[i]
                flag = one if flag is None else jnp.logical_and(flag, one)
        return flag

    def device(move):
        return {NAMES[i]: at[i] + move[i] for i in range(3) if move[i]}

    def opposite(move):
        return tuple(-m for m in move)

    loads = [
        pltpu.make_async_copy(u_in, bar0.at[0, 1 : NZ + 1, 8 : 8 + NY, :], in_sem.at[0]),
        pltpu.make_async_copy(v_in, bar0.at[1:4, 1 : NZ + 1, 8 : 8 + NY, :], in_sem.at[1]),
        pltpu.make_async_copy(p_in, p.at[:, 1 : NZ + 1, 8 : 8 + NY, :], in_sem.at[2]),
        pltpu.make_async_copy(q_in, q.at[:, 0:NZ, 0:NY, :], in_sem.at[3]),
        pltpu.make_async_copy(f_in, fa, in_sem.at[4]),
        pltpu.make_async_copy(w_in, wb, in_sem.at[5]),
    ]
    barrier = pltpu.get_barrier_semaphore()
    arrivals = jnp.int32(0)
    for m in ALL:
        move = MOVES[m]
        arrivals = arrivals + exists(move).astype(jnp.int32)

        @pl.when(exists(move))
        def _():
            pl.semaphore_signal(
                barrier, inc=1, device_id=device(move), device_id_type=pl.DeviceIdType.MESH
            )

    for c in loads:
        c.start()

    def ends(m, r):
        bar = bars[r]
        inner = slice(1, NZ + 1)
        if m == ZUP:
            return bar.at[:, NZ, 8 : 8 + NY, :], bar.at[:, 0, 8 : 8 + NY, :]
        if m == ZDN:
            return bar.at[:, 1, 8 : 8 + NY, :], bar.at[:, NZ + 1, 8 : 8 + NY, :]
        if m == YUP:
            return bar.at[:, 1 : NZ + 1, 7 + NY, :], bar.at[:, 1 : NZ + 1, 7, :]
        if m == YDN:
            return bar.at[:, 1 : NZ + 1, 8, :], bar.at[:, 1 : NZ + 1, 8 + NY, :]
        if m == YUP_ZDN:
            return bar.at[:, 1, 7 + NY, :], bar.at[:, NZ + 1, 7, :]
        if m == YDN_ZUP:
            return bar.at[:, NZ, 8, :], bar.at[:, 0, 8 + NY, :]
        if m == PZ:
            return pzk, p.at[:, 0, 8 : 8 + NY, :]
        if m == QZ:
            return qzk, q.at[:, NZ, 0:NY, :]
        if m == PY:
            return pyk, p.at[:, 1 : NZ + 1, 7, :]
        if m == QY:
            return qyk, q.at[:, 0:NZ, NY, :]
        if m == XUP_YDN:
            return xey.at[r, 0, :, 0, :], d_xmyp.at[r, :, 7, :]
        if m == XDN_YUP:
            return xey.at[r, 1, :, 7, :], d_xpym.at[r, :, 0, :]
        if m == PX_:
            return pxk, plxk
        if m == QX_:
            return qxk, quxk
        src, dst = {
            XUP: (xe, xh_lo), XDN: (xe, xh_hi),
            XUP_ZDN: (xe, d_xmzp), XDN_ZUP: (xe, d_xpzm),
        }[m]
        return src.at[r], dst.at[r]

    def message(m, r):
        src, dst = ends(m, r)
        return pltpu.make_async_remote_copy(
            src_ref=src, dst_ref=dst, send_sem=send_sem.at[r, m], recv_sem=recv_sem.at[r, m],
            device_id=device(MOVES[m]), device_id_type=pl.DeviceIdType.MESH,
        )

    def send(r, which):
        for m in which:
            @pl.when(exists(MOVES[m]))
            def _():
                message(m, r).start()

    def sent(r):
        for m in ALL0 if r == 0 else ALL:
            @pl.when(exists(MOVES[m]))
            def _():
                message(m, r).wait_send()

    def receive(r, which):
        for m in which:
            @pl.when(exists(opposite(MOVES[m])))
            def _():
                message(m, r).wait_recv()

    lane, sub = tile_iota(1), tile_iota(0)
    first, last = lane == 0, lane == 127
    edge = jnp.logical_or(first, last)
    zero = jnp.zeros((8, 128), F32)
    masks = edge_masks(up, down)

    def pack_into(acc, z, t, values, mask, by):
        for f, x in enumerate(values):
            acc[f // 2] = acc[f // 2] + lanes(jnp.where(mask, x, 0.0), (f % 2) * 64 + 2 * (z * TILES + t) + by)

    loads[0].wait()
    loads[1].wait()
    acc = [zero, zero]
    for t in OUTER + INNER:
        for z in range(NZ):
            pack_into(acc, z, t, [bar0[f, z + 1, 8 + 8 * t : 16 + 8 * t, :] for f in range(4)], edge, 0)
    for h in range(2):
        xe[0, h] = acc[h]
        xey[0, 0, h] = lanes(acc[h], CORNER[0])
        xey[0, 1, h] = lanes(acc[h], CORNER[1])
    loads[2].wait()
    loads[3].wait()
    for c in range(3):
        pyk[c] = line(p, c, 1, 7 + NY)
        pzk[c] = p[c, NZ, 8 : 8 + NY, :]
    for i in range(6):
        qyk[i] = line(q, i, 0, 0)
        qzk[i] = q[i, 0, 0:NY, :]
    accp, accq = [zero, zero], [zero, zero, zero]
    for t in EVERY:
        for z in range(NZ):
            pack_into(accp, z, t, [p[a, z + 1, 8 + 8 * t : 16 + 8 * t, :] for a in range(3)], last, 1)
            pack_into(accq, z, t, [q[i, z, 8 * t : 8 * t + 8, :] for i in range(6)], first, 0)
    for h in range(2):
        pxk[h] = accp[h]
    for h in range(3):
        qxk[h] = accq[h]

    pl.semaphore_wait(barrier, arrivals)
    send(0, ALL0)

    loads[4].wait()
    loads[5].wait()
    for z in range(NZ):
        for t in EVERY:
            rows = slice(8 * t, 8 * t + 8)
            tw = TAU * wb[z, rows, :]
            fa[z, rows, :] = tw * fa[z, rows, :]
            wb[z, rows, :] = 1.0 / (1.0 + tw)

    def split(x):
        return [x[0], lanes(x[0], 64), x[1], lanes(x[1], 64)]

    def clamp_x(r):
        @pl.when(jnp.logical_not(up[0]))
        def _():
            for h in range(2):
                xh_hi[r, h] = lanes(xe[r, h], 1)

        @pl.when(jnp.logical_not(down[0]))
        def _():
            for h in range(2):
                xh_lo[r, h] = lanes(xe[r, h], -1)

    def clamp_z(r):
        bar = bars[r]

        @pl.when(jnp.logical_not(up[2]))
        def _():
            bar[:, NZ + 1, 8 : 8 + NY, :] = bar[:, NZ, 8 : 8 + NY, :]

        @pl.when(jnp.logical_not(down[2]))
        def _():
            bar[:, 0, 8 : 8 + NY, :] = bar[:, 1, 8 : 8 + NY, :]

    def clamp_lower(r):
        bar = bars[r]

        @pl.when(jnp.logical_not(up[2]))
        def _():
            for f in range(4):
                bar[f, NZ + 1, 7:8, :] = bar[f, NZ, 7:8, :]

        @pl.when(jnp.logical_not(down[1]))
        def _():
            for f in range(4):
                bar[f, NZ + 1, 7:8, :] = bar[f, NZ + 1, 8:9, :]
                flat(bar)[f, steps(bar, 1, 7), :] = line(bar, f, 1, 8)

    def clamp_upper(r):
        bar = bars[r]

        @pl.when(jnp.logical_not(down[2]))
        def _():
            for f in range(4):
                bar[f, 0, 8 + NY : 9 + NY, :] = bar[f, 1, 8 + NY : 9 + NY, :]

        @pl.when(jnp.logical_not(up[1]))
        def _():
            for f in range(4):
                bar[f, 0, 8 + NY : 9 + NY, :] = bar[f, 0, 7 + NY : 8 + NY, :]
                flat(bar)[f, steps(bar, 1, 8 + NY), :] = line(bar, f, 1, 7 + NY)

    in64 = lax.rem(lane, 64)
    in8 = lax.rem(lane, 8)

    def x_below(r, corners):
        if not corners:
            low = [lanes(xh_lo[r, h], 1) for h in range(2)]
            a = subs(low[0], -1)
            for k, x in enumerate(split(low)):
                early[k] = x
            early[4] = jnp.where(sub < 7, a, jnp.where(in8 < 6, lanes(a, -2), low[0]))
            early[5] = jnp.where(in64 < 56, lanes(low[0], -8), jnp.where(up[2], lanes(d_xmzp[r, 0], 57), low[0]))
        ny = early[4]
        if corners:
            at_edge = jnp.logical_and(jnp.logical_and(sub == 7, in8 >= 6), up[1])
            ny = jnp.where(at_edge, d_xmyp[r, 0], ny)
        new = p_step([plx[c] for c in range(3)], early[0], [xe[r, 0], ny, early[5]], [early[1 + c] for c in range(3)])
        if corners:
            for c in range(3):
                plx[c] = new[c]
        return jnp.where(down[0], new[0], zero)

    def x_above(r, corners):
        if not corners:
            high = [xh_hi[r, h] for h in range(2)]
            py_, pz_ = [], []
            for h in range(2):
                a = subs(high[h], 1)
                py_.append(jnp.where(sub > 0, a, jnp.where(in8 >= 2, lanes(a, 2), high[h])))
                pz_.append(jnp.where(in64 >= 8, lanes(high[h], 8),
                                     jnp.where(down[2], lanes(d_xpzm[r, h], -56), high[h])))
            for k, x in enumerate((high, [lanes(xe[r, h], 1) for h in range(2)], py_, pz_)):
                for c, y in enumerate(split(x)[1:]):
                    early[6 + 3 * k + c] = y
        v, own, py_, pz_ = [[early[6 + 3 * k + c] for c in range(3)] for k in range(4)]
        if corners:
            at_edge = jnp.logical_and(jnp.logical_and(sub == 0, in8 < 2), down[1])
            corner = split([d_xpym[r, h] for h in range(2)])[1:]
            py_ = [jnp.where(at_edge, corner[c], py_[c]) for c in range(3)]
        new = q_step([qux[i] for i in range(6)], v, [own, py_, pz_])
        if corners:
            for i in range(6):
                qux[i] = new[i]
        return [jnp.where(up[0], new[i], zero) for i in Q_OF[0]]

    def column(source, row, base):
        line_ = jnp.broadcast_to(source[row : row + 1, :], (8, 128))
        picked = jnp.where(lane == lax.rem(8 * sub + base % 128, 128), line_, 0.0)
        return jnp.broadcast_to(jnp.sum(picked, axis=1, keepdims=True), (8, 128))

    def keep_rows(r):
        for c in range(3):
            kept[c] = line(p, c, 1, 7 + NY)
            kept[10 + c] = column(xh_lo.at[r, (1 + c) // 2], 0, ((1 + c) % 2) * 64 - 1)
        for i in range(6):
            kept[3 + i] = line(q, i, 0, 0)
        kept[9] = column(xh_hi.at[r, 0], 7, 6)

    def redo_upper(r):
        bar = bars[r]
        here = line(bar, 0, 1, 7 + NY)
        nx = jnp.where(last, kept[9], lanes(here, -1))
        new = p_step([kept[c] for c in range(3)], here, [nx, line(bar, 0, 1, 8 + NY), line(bar, 0, 2, 7 + NY)],
                     [line(bar, 1 + c, 1, 7 + NY) for c in range(3)])
        for c in range(3):
            flat(p)[c, steps(p, 1, 7 + NY), :] = new[c]

    def redo_lower(r):
        bar = bars[r]
        v = [line(bar, 1 + c, 1, 8) for c in range(3)]
        bx = [jnp.where(first, kept[10 + c], lanes(v[c], 1)) for c in range(3)]
        new = q_step([kept[3 + i] for i in range(6)], v,
                     [bx, [line(bar, 1 + c, 1, 7) for c in range(3)], [line(bar, 1 + c, 0, 8) for c in range(3)]])
        for i in range(6):
            flat(q)[i, steps(q, 0, 0), :] = new[i]

    def y_below(r):
        bar = bars[r]
        here = line(bar, 0, 1, 7)
        nx = jnp.where(lane < 127, lanes(here, -1), jnp.where(up[0], column(d_xpym.at[r, 0], 0, 6 + CORNER[1]), here))
        new = p_step([line(p, c, 1, 7) for c in range(3)], here,
                     [nx, line(bar, 0, 1, 8), line(bar, 0, 2, 7)], [line(bar, 1 + c, 1, 7) for c in range(3)])
        new[1] = jnp.where(down[1], new[1], zero)
        for c in range(3):
            flat(p)[c, steps(p, 1, 7), :] = new[c]

    def y_above(r):
        bar = bars[r]
        v = [line(bar, 1 + c, 1, 8 + NY) for c in range(3)]
        bx = [jnp.where(lane > 0, lanes(v[c], 1), jnp.where(down[0], column(d_xmyp.at[r, (1 + c) // 2], 7, ((1 + c) % 2) * 64 - 1 + CORNER[0]), v[c]))
              for c in range(3)]
        new = q_step([line(q, i, 0, NY) for i in range(6)], v,
                     [bx, [line(bar, 1 + c, 1, 7 + NY) for c in range(3)],
                      [line(bar, 1 + c, 0, 8 + NY) for c in range(3)]])
        for i in range(6):
            flat(q)[i, steps(q, 0, NY), :] = jnp.where(up[1], new[i], zero) if i in Q_OF[1] else new[i]

    def z_below(r, tiles):
        bar = bars[r]
        for t in tiles:
            rows = slice(8 + 8 * t, 16 + 8 * t)
            here = bar[0, 0, rows, :]
            nx = jnp.where(lane < 127, lanes(here, -1),
                           jnp.where(up[0], lanes(d_xpzm[r, 0], 127 - 56 - 2 * t), here))
            new = p_step([p[c, 0, rows, :] for c in range(3)], here,
                         [nx, bar[0, 0, 9 + 8 * t : 17 + 8 * t, :], bar[0, 1, rows, :]],
                         [bar[1 + c, 0, rows, :] for c in range(3)])
            new[2] = jnp.where(down[2], new[2], zero)
            for c in range(3):
                p[c, 0, rows, :] = new[c]

    def z_above(r, tiles):
        bar = bars[r]
        for t in tiles:
            rows = slice(8 + 8 * t, 16 + 8 * t)
            v = [bar[1 + c, NZ + 1, rows, :] for c in range(3)]
            bx = [jnp.where(lane > 0, lanes(v[c], 1),
                            jnp.where(down[0], lanes(d_xmzp[r, (1 + c) // 2], -((1 + c) % 2) * 64 - 2 * t + 1), v[c]))
                  for c in range(3)]
            new = q_step([q[i, NZ, 8 * t : 8 * t + 8, :] for i in range(6)], v,
                         [bx, [bar[1 + c, NZ + 1, 7 + 8 * t : 15 + 8 * t, :] for c in range(3)],
                          [bar[1 + c, NZ, rows, :] for c in range(3)]])
            for i in range(6):
                q[i, NZ, 8 * t : 8 * t + 8, :] = jnp.where(up[2], new[i], zero) if i in Q_OF[2] else new[i]

    def dual(r, slabs):
        bar = bars[r]
        high = xh_hi[r, 0]
        low = [xh_lo[r, h] for h in range(2)]
        for z in slabs:
            for t in EVERY:
                rows = slice(8 + 8 * t, 16 + 8 * t)
                mine = slice(8 * t, 8 * t + 8)
                s = z * TILES + t
                here = bar[0, z + 1, rows, :]
                v = [bar[1 + c, z + 1, rows, :] for c in range(3)]
                nx = jnp.where(last, lanes(high, 127 - 2 * s), lanes(here, -1))
                ny = subs(here, -1) if t == TILES - 1 else bar[0, z + 1, 9 + 8 * t : 17 + 8 * t, :]
                by = [subs(v[c], 1) if t == 0 else bar[1 + c, z + 1, 7 + 8 * t : 15 + 8 * t, :] for c in range(3)]
                new = p_step([p[c, z + 1, rows, :] for c in range(3)], here,
                             [nx, ny, bar[0, z + 2, rows, :]], v)
                for c in range(3):
                    p[c, z + 1, rows, :] = new[c]
                bx = [jnp.where(first, lanes(low[(1 + c) // 2], 1 - ((1 + c) % 2) * 64 - 2 * s), lanes(v[c], 1))
                      for c in range(3)]
                new = q_step([q[i, z, mine, :] for i in range(6)], v,
                             [bx, by, [bar[1 + c, z, rows, :] for c in range(3)]])
                for i in range(6):
                    q[i, z, mine, :] = new[i]

    def primal(r, tiles, acc, below_x, above_x, by=0):
        for t in tiles:
            for z in range(NZ):
                rows = slice(8 + 8 * t, 16 + 8 * t)
                mine = slice(8 * t, 8 * t + 8)
                if r == 0:
                    old = [bar0[f, z + 1, rows, :] for f in range(4)]
                else:
                    old = [uv[f, z, mine, :] for f in range(4)]
                new, values = primal_tile(z, t, masks, p, q, old, (fa[z, mine, :], wb[z, mine, :]), below_x, above_x)
                for f in range(4):
                    uv[f, z, mine, :] = new[f]
                    if r < ITERS - 1:
                        bars[r + 1][f, z + 1, rows, :] = values[f]
                if r < ITERS - 1:
                    pack_into(acc, z, t, values, edge, by)

    low_side = at[1] < sizes[1] // 2
    for r in range(ITERS):
        start, more = r == 0, r < ITERS - 1
        receive(r, ALONG_X0 if start else ALONG_X)
        clamp_x(r)
        if start:
            for c in range(3):
                plx[c] = lanes(plxk[c // 2], (c % 2) * 64)
            for i in range(6):
                qux[i] = lanes(quxk[i // 2], (i % 2) * 64)
        keep_rows(r)
        dual(r, range(1, NZ - 1))
        receive(r, ALONG_Z0 if start else ALONG_Z)
        clamp_z(r)
        dual(r, (0, NZ - 1))
        z_below(r, EVERY[:-1])
        z_above(r, EVERY[1:])
        below_x, above_x = x_below(r, False), x_above(r, False)
        acc = [zero, zero]
        primal(r, INNER, acc, below_x, above_x)
        if r > 0:
            sent(r - 1)
        for h in range(2):
            xei[h] = acc[h]
        cols[0] = below_x
        for j in range(3):
            cols[1 + j] = above_x[j]

        def border(t, below, above, side, sends):
            acc = [zero, zero]
            primal(r, (t,), acc, below, above, CORNER[side])
            for h in range(2):
                xey[r + 1, side, h] = acc[h]
            send(r + 1, sends)

        def lower():
            receive(r, LOWER0 if start else LOWER)
            clamp_lower(r)
            above = x_above(r, True)
            y_below(r)
            z_above(r, (0,))
            redo_lower(r)
            if more:
                border(0, cols[0], above, 0, UPPER)
            else:
                for j in range(3):
                    cols[4 + j] = above[j]

        def upper():
            receive(r, UPPER0 if start else UPPER)
            clamp_upper(r)
            below = x_below(r, True)
            y_above(r)
            z_below(r, (TILES - 1,))
            redo_upper(r)
            if more:
                border(TILES - 1, below, [cols[1 + j] for j in range(3)], 1, LOWER)
            else:
                cols[7] = below

        @pl.when(low_side)
        def _():
            lower()
            upper()

        @pl.when(jnp.logical_not(low_side))
        def _():
            upper()
            lower()

        if more:
            for h in range(2):
                xe[r + 1, h] = xei[h] + (lanes(xey[r + 1, 0, h], -CORNER[0]) + lanes(xey[r + 1, 1, h], -CORNER[1]))
            send(r + 1, ALONG_X + ALONG_Z)
    sent(ITERS - 1)


def final_kernel(sizes, uv, p, q, fa, wb, cols, u_out, v_out, p_out, q_out, new_uv, out_sem):
    _, up, down = place(sizes)
    masks = edge_masks(up, down)
    stores = [
        pltpu.make_async_copy(p.at[:, 1 : NZ + 1, 8 : 8 + NY, :], p_out, out_sem.at[0]),
        pltpu.make_async_copy(q.at[:, 0:NZ, 0:NY, :], q_out, out_sem.at[1]),
    ]
    for c in stores:
        c.start()
    middle = slice(8, NY - 8)
    more = [
        pltpu.make_async_copy(uv.at[0, :, middle, :], u_out.at[:, middle, :], out_sem.at[2]),
        pltpu.make_async_copy(uv.at[1:4, :, middle, :], v_out.at[:, :, middle, :], out_sem.at[3]),
    ]
    for c in more:
        c.start()
    stores += more
    for k, t in enumerate(OUTER):
        mine = slice(8 * t, 8 * t + 8)
        for z in range(NZ):
            new, _ = primal_tile(z, t, masks, p, q, [uv[f, z, mine, :] for f in range(4)],
                                 (fa[z, mine, :], wb[z, mine, :]), cols[7 * k],
                                 [cols[4 - 3 * k + j] for j in range(3)])
            for f in range(4):
                new_uv[k, f, z] = new[f]
        more = [
            pltpu.make_async_copy(new_uv.at[k, 0], u_out.at[:, mine, :], out_sem.at[4 + k]),
            pltpu.make_async_copy(new_uv.at[k, 1:4], v_out.at[:, :, mine, :], out_sem.at[6 + k]),
        ]
        for c in more:
            c.start()
        stores += more
    for c in stores:
        c.wait()


def per_device(sizes, *arrays):
    hbm = pl.BlockSpec(memory_space=pltpu.HBM)
    here = pl.BlockSpec(memory_space=pltpu.VMEM)
    tile = (8, 128)

    def vmem(*shape):
        return pltpu.VMEM(shape, F32)

    state = pl.pallas_call(
        functools.partial(exchange_kernel, sizes),
        out_shape=(
            vmem(4, NZ, NY, NX),
            vmem(3, NZ + 1, PROWS, NX),
            vmem(6, NZ + 1, PROWS, NX),
            vmem(NZ, NY, NX),
            vmem(NZ, NY, NX),
            vmem(8, *tile),
        ),
        in_specs=[hbm] * 6,
        out_specs=(here,) * 6,
        scratch_shapes=[
            vmem(4, NZ + 2, ROWS, NX), vmem(4, NZ + 2, ROWS, NX), vmem(4, NZ + 2, ROWS, NX),
            vmem(ITERS, 2, *tile), vmem(ITERS, 2, 2, *tile), vmem(2, *tile), vmem(13, *tile), vmem(18, *tile),
            vmem(ITERS, 2, *tile), vmem(ITERS, 2, *tile),
            vmem(ITERS, 2, *tile), vmem(ITERS, 2, *tile), vmem(ITERS, 2, *tile), vmem(ITERS, 2, *tile),
            vmem(2, *tile), vmem(3, *tile), vmem(3, *tile), vmem(6, *tile), vmem(3, NY, NX), vmem(6, NY, NX),
            vmem(2, *tile), vmem(3, *tile),
            vmem(3, *tile), vmem(6, *tile),
            pltpu.SemaphoreType.DMA((6,)),
            pltpu.SemaphoreType.DMA((ITERS, 18)),
            pltpu.SemaphoreType.DMA((ITERS, 18)),
        ],
        compiler_params=pltpu.CompilerParams(
            collective_id=0, has_side_effects=True, vmem_limit_bytes=24 << 20
        ),
        name="tgv_rounds",
    )(*[pltpu.with_memory_space_constraint(a, pltpu.HBM) for a in arrays])
    return pl.pallas_call(
        functools.partial(final_kernel, sizes),
        out_shape=tuple(jax.ShapeDtypeStruct(s, F32) for s in
                        ((NZ, NY, NX), (3, NZ, NY, NX), (3, NZ, NY, NX), (6, NZ, NY, NX))),
        in_specs=[here] * 6,
        out_specs=(hbm,) * 4,
        scratch_shapes=[vmem(2, 4, NZ, *tile), pltpu.SemaphoreType.DMA((8,))],
        compiler_params=pltpu.CompilerParams(vmem_limit_bytes=24 << 20),
        name="tgv_last",
    )(*state)


def solution(mesh):
    sizes = tuple(mesh.shape[n] for n in NAMES)
    scalar = P("gz", "gy", "gx")
    stack = P(None, "gz", "gy", "gx")
    return jax.shard_map(
        functools.partial(per_device, sizes), mesh=mesh,
        in_specs=(scalar, scalar, scalar, stack, stack, stack),
        out_specs=(scalar, stack, stack, stack), check_vma=False,
    )
```
